32 devices in a mesh: dp: 1 (over z), tp: 4 (over y), wg: 8 (over x, core).
Axes of the slice: x: 4, y: 4, z: 1, core: 2. Of those that a mesh axis runs over, the one named last changes fastest.
The devices are a block of a 4x4x8 slice.
Arguments:
- tokens: bfloat16 [1024, 2560], P(('dp', 'wg'))
- gain_attn: float32 [2560], P('wg')
- gain_mlp: float32 [2560], P('wg')
- w_qkv: bfloat16 [2560, 3, 32, 80], P('wg', None, 'tp')
- w_rel: bfloat16 [2560, 32, 80], P('wg', 'tp')
- w_out: bfloat16 [32, 80, 2560], P('tp', None, 'wg')
- w_up: bfloat16 [2560, 10240], P('wg', 'tp')
- w_down: bfloat16 [10240, 2560], P('tp', 'wg')
- bias_u: float32 [32, 80], P('tp')
- bias_v: float32 [32, 80], P('tp')
- rel_table: bfloat16 [16, 2560], replicated
- k_cache: bfloat16 [1024, 32, 16, 80], P(('dp', 'wg'), 'tp')
- v_cache: bfloat16 [1024, 32, 16, 80], P(('dp', 'wg'), 'tp')
- positions: int32 [1024], P(('dp', 'wg'))
Outputs:
- output 1: bfloat16 [1024, 2560], P(('dp', 'wg'))
- output 2: bfloat16 [1024, 32, 80], P(('dp', 'wg'), 'tp')
- output 3: bfloat16 [1024, 32, 80], P(('dp', 'wg'), 'tp')
All inputs are finite; a program needn't handle non-finite values.
Results may differ from the reference program's by a relative error of at most 0.0133234.
Values are sent between devices in bfloat16 or wider.
A program may use at most 768 MiB of HBM per device.

```python
import math
import jax
import jax.numpy as jnp
from jax import lax

D_MODEL = 2560
N_HEADS = 32
HEAD_DIM = 80
FF_DIM = 10240
CACHE_LEN = 16
SEQ_COUNT = 1024
SEQ_BLOCK = 8
NORM_EPS = 1e-6
SCORE_SCALE = 1.0 / math.sqrt(HEAD_DIM)
BLOCK_COUNT = SEQ_COUNT // SEQ_BLOCK


def setup_inputs(seed: int = 0, part: int = 0) -> dict:
    base_key = jax.random.key(seed)
    part_key = jax.random.fold_in(base_key, part)
    weight_keys = jax.random.split(base_key, 12)
    part_keys = jax.random.split(part_key, 4)
    head_width = N_HEADS * HEAD_DIM
    gain_attn = jax.random.uniform(weight_keys[0], (D_MODEL,), jnp.float32, 0.5, 1.5)
    gain_mlp = jax.random.uniform(weight_keys[1], (D_MODEL,), jnp.float32, 0.5, 1.5)
    w_qkv = (jax.random.normal(weight_keys[2], (D_MODEL, 3, N_HEADS, HEAD_DIM), jnp.float32) * D_MODEL ** -0.5).astype(jnp.bfloat16)
    w_rel = (jax.random.normal(weight_keys[3], (D_MODEL, N_HEADS, HEAD_DIM), jnp.float32) * (2.0 / D_MODEL) ** 0.5).astype(jnp.bfloat16)
    w_out = (jax.random.normal(weight_keys[4], (N_HEADS, HEAD_DIM, D_MODEL), jnp.float32) * 2.0 * head_width ** -0.5).astype(jnp.bfloat16)
    w_up = (jax.random.normal(weight_keys[5], (D_MODEL, FF_DIM), jnp.float32) * D_MODEL ** -0.5).astype(jnp.bfloat16)
    w_down = (jax.random.normal(weight_keys[6], (FF_DIM, D_MODEL), jnp.float32) * FF_DIM ** -0.5).astype(jnp.bfloat16)
    bias_u = jax.random.normal(weight_keys[7], (N_HEADS, HEAD_DIM), jnp.float32)
    bias_v = jax.random.normal(weight_keys[8], (N_HEADS, HEAD_DIM), jnp.float32)
    rel_freqs = jnp.exp(jax.random.uniform(weight_keys[9], (D_MODEL,), jnp.float32, math.log(0.01), math.log(3.0)))
    phases = jax.random.uniform(weight_keys[10], (D_MODEL,), jnp.float32, 0.0, 2.0 * math.pi)
    offsets = jnp.arange(CACHE_LEN, dtype=jnp.float32)
    rel_table = jnp.sin(offsets[:, None] * rel_freqs[None, :] + phases[None, :]).astype(jnp.bfloat16)
    tokens = jax.random.normal(part_keys[0], (SEQ_COUNT, D_MODEL), jnp.float32).astype(jnp.bfloat16)
    k_cache = jax.random.normal(part_keys[1], (SEQ_COUNT, N_HEADS, CACHE_LEN, HEAD_DIM), jnp.float32).astype(jnp.bfloat16)
    v_cache = jax.random.normal(part_keys[2], (SEQ_COUNT, N_HEADS, CACHE_LEN, HEAD_DIM), jnp.float32).astype(jnp.bfloat16)
    positions = jax.random.randint(part_keys[3], (SEQ_COUNT,), 0, CACHE_LEN, jnp.int32)
    positions = positions.at[0].set(CACHE_LEN - 1)
    return {"tokens": tokens, "gain_attn": gain_attn, "gain_mlp": gain_mlp, "w_qkv": w_qkv, "w_rel": w_rel, "w_out": w_out, "w_up": w_up, "w_down": w_down, "bias_u": bias_u, "bias_v": bias_v, "rel_table": rel_table, "k_cache": k_cache, "v_cache": v_cache, "positions": positions}


def rms_norm(row_vals, gain_vec):
    vals_f32 = row_vals.astype(jnp.float32)
    mean_sq = jnp.mean(vals_f32 * vals_f32, axis=-1, keepdims=True)
    return (vals_f32 * lax.rsqrt(mean_sq + NORM_EPS) * gain_vec).astype(jnp.bfloat16)


def attend_block(block_args, rel_f32):
    q_u, q_v, k_new, v_new, k_blk, v_blk, pos_blk = block_args
    key_steps = jnp.arange(CACHE_LEN)
    is_self = key_steps[None, :] == pos_blk[:, None]
    is_valid = key_steps[None, :] <= pos_blk[:, None]
    k_full = jnp.where(is_self[:, None, :, None], k_new[:, :, None, :], k_blk).astype(jnp.float32)
    v_full = jnp.where(is_self[:, None, :, None], v_new[:, :, None, :], v_blk).astype(jnp.float32)
    content = jnp.einsum("bhe,bhje->bhj", q_u.astype(jnp.float32), k_full)
    rel_all = jnp.einsum("bhe,rhe->bhr", q_v.astype(jnp.float32), rel_f32)
    rel_index = jnp.clip(pos_blk[:, None] - key_steps[None, :], 0, CACHE_LEN - 1)
    rel_scores = jnp.take_along_axis(rel_all, jnp.broadcast_to(rel_index[:, None, :], rel_all.shape), axis=2)
    scores = jnp.where(is_valid[:, None, :], (content + rel_scores) * SCORE_SCALE, -1e30)
    attn_probs = jax.nn.softmax(scores, axis=-1).astype(jnp.bfloat16)
    attn_out = jnp.einsum("bhj,bhje->bhe", attn_probs.astype(jnp.float32), v_full)
    return attn_out.astype(jnp.bfloat16)


def reference(tokens, gain_attn, gain_mlp, w_qkv, w_rel, w_out, w_up, w_down, bias_u, bias_v, rel_table, k_cache, v_cache, positions):
    head_width = N_HEADS * HEAD_DIM
    normed = rms_norm(tokens, gain_attn)
    qkv_heads = jnp.dot(normed, w_qkv.reshape(D_MODEL, 3 * head_width), preferred_element_type=jnp.float32).astype(jnp.bfloat16).reshape(SEQ_COUNT, 3, N_HEADS, HEAD_DIM)
    q_heads = qkv_heads[:, 0]
    k_new = qkv_heads[:, 1]
    v_new = qkv_heads[:, 2]
    rel_proj = jnp.dot(rel_table, w_rel.reshape(D_MODEL, head_width), preferred_element_type=jnp.float32).astype(jnp.bfloat16).reshape(CACHE_LEN, N_HEADS, HEAD_DIM)
    rel_f32 = rel_proj.astype(jnp.float32)
    q_u = (q_heads.astype(jnp.float32) + bias_u).astype(jnp.bfloat16)
    q_v = (q_heads.astype(jnp.float32) + bias_v).astype(jnp.bfloat16)

    def to_blocks(array_in):
        return array_in.reshape((BLOCK_COUNT, SEQ_BLOCK) + array_in.shape[1:])

    def run_block(block_args):
        return attend_block(block_args, rel_f32)

    blocked = tuple(to_blocks(array_in) for array_in in (q_u, q_v, k_new, v_new, k_cache, v_cache, positions))
    attn_out = lax.map(run_block, blocked)
    attn_flat = attn_out.reshape(SEQ_COUNT, head_width)
    attn_proj = jnp.dot(attn_flat, w_out.reshape(head_width, D_MODEL), preferred_element_type=jnp.float32)
    resid = tokens.astype(jnp.float32) + attn_proj
    normed_mlp = rms_norm(resid, gain_mlp)
    hidden = jax.nn.gelu(jnp.dot(normed_mlp, w_up, preferred_element_type=jnp.float32), approximate=True).astype(jnp.bfloat16)
    layer_out = (resid + jnp.dot(hidden, w_down, preferred_element_type=jnp.float32)).astype(jnp.bfloat16)
    return (layer_out, k_new, v_new)
```

```python
import functools
import math

import jax
import jax.numpy as jnp
from jax import lax
from jax.experimental import pallas as pl
from jax.experimental.pallas import tpu as pltpu
from jax.sharding import PartitionSpec as P

MESH = pl.DeviceIdType.MESH
NORM_EPS = 1e-6
BF16 = jnp.bfloat16
F32 = jnp.float32
NT = (((1,), (1,)), ((), ()))
NN = (((1,), (0,)), ((), ()))
N_REMOTE = 160
N_LOCAL = 32


def dot(a, b, dims):
    return lax.dot_general(a, b, dims, preferred_element_type=F32)


def layer_kernel(nx, ny, tok_ref, ga_ref, gm_ref, wqkv_ref, wrel_ref, wout_ref, wup_ref, wdn_ref, bu_ref, bv_ref, relt_ref, kc_ref, vc_ref, pos_ref,
                 y_ref, kn_ref, vn_ref,
                 xall, nall, gall, gmx, wq_land, wq, qst, qin, kc, vc, wrel, rsend, rland, s_ref, p_ref, o_t, oall, wo_land, wo,
                 st1, in1, hbuf, st_s, st_r, mall, wup, zall, wdn, st2, in2, yst, yfull,
                 ss, rs, ls):
    w = lax.axis_index("wg")
    x, c, y = w // 2, w % 2, lax.axis_index("tp")
    rows, d_model = tok_ref.shape
    ds = ga_ref.shape[1]
    dx = 2 * ds
    n_heads, n_slots, hd, _ = kc_ref.shape
    hx = n_heads // nx
    fx = wup_ref.shape[1] // nx
    qr = rows // ny
    hw = n_heads * hd

    def dev(xx, cc, yy):
        return {"wg": 2 * xx + cc, "tp": yy}

    def xp(i):
        return lax.rem(x + i, nx)

    def yp(i):
        return lax.rem(y + i, ny)

    sib = dev(x, 1 - c, y)
    counter = [0, 0]
    pending = []

    def new():
        counter[0] += 1
        return counter[0] - 1

    def send(src, dst, to, i):
        cp = pltpu.make_async_remote_copy(src_ref=src, dst_ref=dst, send_sem=ss.at[i], recv_sem=rs.at[i], device_id=to, device_id_type=MESH)
        cp.start()
        pending.append(cp)

    def arrived(dst, i):
        pltpu.make_async_remote_copy(src_ref=dst, dst_ref=dst, send_sem=ss.at[i], recv_sem=rs.at[i], device_id=sib, device_id_type=MESH).wait_recv()

    def local(src, dst):
        cp = pltpu.make_async_copy(src, dst, ls.at[counter[1]])
        counter[1] += 1
        cp.start()
        return cp

    def xlane(ref_cols, xx):
        return pl.ds(pl.multiple_of(xx * ref_cols, 128), ref_cols)

    def qrow(yy):
        return pl.ds(pl.multiple_of(yy * qr, qr), qr)

    xs, ys = range(1, nx), range(1, ny)

    c_x = local(tok_ref, xall.at[x])
    c_wq = local(wqkv_ref.at[:, pl.ds(x * hx, hx)], wq_land.at[w])
    c_rel = local(wrel_ref, wrel)
    c_ga = local(ga_ref, gall.at[w])
    c_gm = local(gm_ref, gmx.at[c])
    c_k = local(kc_ref, kc)
    c_v = local(vc_ref, vc)
    c_wo = local(wout_ref, wo_land.at[c])
    c_up = local(wup_ref.at[:, xlane(fx, x)], wup.at[w])
    c_dn = local(wdn_ref, wdn.at[c])

    barrier = pltpu.get_barrier_semaphore()
    peers = [dev(xp(i), c, y) for i in xs] + [dev(x, c, yp(i)) for i in ys] + [sib] + [dev(xp(i), 1 - c, y) for i in xs]
    for peer in peers:
        pl.semaphore_signal(barrier, inc=1, device_id=peer, device_id_type=MESH)
    pl.semaphore_wait(barrier, len(peers))

    i_tx = {i: new() for i in xs}
    for i in xs:
        send(tok_ref.at[qrow(y)], xall.at[x, qrow(y)], dev(xp(i), c, y), i_tx[i])
    i_ga = {}
    for i in range(nx):
        for f in range(2):
            if i or f:
                i_ga[i, f] = new()
                to = dev(xp(i), lax.rem(c + f, 2), y)
                send(ga_ref, gall.at[w], to, i_ga[i, f])
    i_gm = new()
    send(gm_ref, gmx.at[c], sib, i_gm)
    i_wx = {i: new() for i in xs}
    for i in xs:
        send(wqkv_ref.at[:, pl.ds(xp(i) * hx, hx)], wq_land.at[w], dev(xp(i), c, y), i_wx[i])
    i_ws = {i: new() for i in range(nx)}
    send(wqkv_ref.at[:, pl.ds(x * hx, hx)], wq_land.at[w], sib, i_ws[0])
    c_rel.wait()
    tab = relt_ref[:, xlane(dx, x)]
    tab = jnp.where(c == 0, tab[:, :ds], tab[:, ds:])
    rsend[...] = dot(tab, wrel[...], NT)
    rland[w] = rsend[...]
    i_rel = {}
    for i in range(nx):
        for f in range(2):
            if i or f:
                i_rel[i, f] = new()
                send(rsend, rland.at[w], dev(xp(i), lax.rem(c + f, 2), y), i_rel[i, f])
    i_ty = {(i, k): new() for i in xs for k in ys}
    for i in xs:
        src = lax.rem(x + nx - i, nx)
        blk = xall.at[src, qrow(y)]
        arrived(blk, i_tx[i])
        for k in ys:
            send(blk, blk, dev(x, c, yp(k)), i_ty[i, k])
    i_wo, i_dn = new(), new()
    send(wout_ref, wo_land.at[c], sib, i_wo)
    send(wdn_ref, wdn.at[c], sib, i_dn)
    for i in xs:
        blk = wq_land.at[2 * lax.rem(x + nx - i, nx) + c]
        arrived(blk, i_wx[i])
        send(blk, blk, sib, i_ws[i])
    for i in range(nx):
        for f in range(2):
            if i or f:
                arrived(gall.at[2 * lax.rem(x + nx - i, nx) + lax.rem(c + f, 2)], i_ga[i, f])
    c_ga.wait()
    gain = jnp.concatenate([gall[j] for j in range(2 * nx)], axis=1)
    c_x.wait()
    for i in xs:
        for k in ys:
            arrived(xall.at[lax.rem(x + nx - i, nx), qrow(lax.rem(y + ny - k, ny))], i_ty[i, k])
    blk_rows = 32

    def norm_block(r, carry):
        g = r // (rows // blk_rows)
        b = pl.ds(pl.multiple_of(lax.rem(r, rows // blk_rows) * blk_rows, blk_rows), blk_rows)
        v = xall[g, b, :].astype(F32)
        ms = jnp.mean(v * v, axis=-1, keepdims=True)
        nall[g, b, :] = (v * lax.rsqrt(ms + NORM_EPS) * gain).astype(BF16)
        return carry

    lax.fori_loop(0, nx * rows // blk_rows, norm_block, 0)
    c_wq.wait()
    for i in range(nx):
        arrived(wq_land.at[2 * lax.rem(x + nx - i, nx) + 1 - c], i_ws[i])
    for j in range(nx):
        for s in range(3):
            for e in range(hx):
                pair = jnp.concatenate([wq_land[2 * j, s, e], wq_land[2 * j + 1, s, e]], axis=1)
                wq[(s * hx + e) * hd:(s * hx + e + 1) * hd, j * dx:(j + 1) * dx] = pair
    i_q = {i: new() for i in xs}
    for g in range(nx):
        res = dot(wq[...], nall[g], NT).astype(BF16)
        qst[g] = res.reshape(3, hx, hd, rows)
    for i in xs:
        send(qst.at[xp(i)], qin.at[x], dev(xp(i), c, y), i_q[i])
    qin[x] = qst[x]
    i_ux = {i: new() for i in xs}
    i_us = {i: new() for i in range(nx)}
    send(wup_ref.at[:, xlane(fx, x)], wup.at[w], sib, i_us[0])
    for i in range(nx):
        for f in range(2):
            if i or f:
                arrived(rland.at[2 * lax.rem(x + nx - i, nx) + lax.rem(c + f, 2)], i_rel[i, f])
    rel = rland[0]
    for j in range(1, 2 * nx):
        rel = rel + rland[j]
    rel = rel.astype(BF16).astype(F32)
    rel = jnp.broadcast_to(rel[:, None, :], (n_slots, n_heads, hw)).reshape(n_slots * n_heads, hw)
    col = lax.broadcasted_iota(jnp.int32, rel.shape, 1)
    row_head = lax.rem(lax.broadcasted_iota(jnp.int32, rel.shape, 0), n_heads)
    keep = (col >= row_head * hd) & (col < row_head * hd + hd)
    rel_diag = jnp.where(keep, rel, 0.0).astype(BF16)

    for i in xs:
        arrived(qin.at[lax.rem(x + nx - i, nx)], i_q[i])
    outs = []
    for j in range(nx):
        outs.append(local(qin.at[j, 1], kn_ref.at[j * hx:(j + 1) * hx]))
        outs.append(local(qin.at[j, 2], vn_ref.at[j * hx:(j + 1) * hx]))
    pos = pos_ref[...]
    bu_t, bv_t = bu_ref[...].T, bv_ref[...].T
    scale = 1.0 / math.sqrt(hd)
    c_k.wait()
    selfs, qvs = [], []
    for h in range(n_heads):
        q = qin[h // hx, 0, h % hx].astype(F32)
        qu = (q + bu_t[:, h:h + 1]).astype(BF16).astype(F32)
        qvs.append((q + bv_t[:, h:h + 1]).astype(BF16))
        selfs.append(jnp.sum(qu * qin[h // hx, 1, h % hx].astype(F32), axis=0, keepdims=True))
        for j in range(n_slots):
            s_ref[j, h:h + 1, :] = jnp.sum(kc[h, j].astype(F32) * qu, axis=0, keepdims=True)
    self_score = jnp.concatenate(selfs, axis=0)
    rel_all = dot(rel_diag, jnp.concatenate(qvs, axis=0), NN)
    rel_all = [rel_all[r * n_heads:(r + 1) * n_heads] for r in range(n_slots)][::-1]
    shift = n_slots - 1 - pos
    bit = 1
    while bit < n_slots:
        take = (shift // bit) % 2 == 1
        rel_all = [jnp.where(take, rel_all[j + bit], rel_all[j]) if j + bit < n_slots else rel_all[j] for j in range(n_slots)]
        bit *= 2
    sc = []
    for j in range(n_slots):
        content = jnp.where(pos == j, self_score, s_ref[j])
        sc.append(jnp.where(pos >= j, (content + rel_all[j]) * scale, -1e30))
    top = functools.reduce(jnp.maximum, sc)
    ex = [jnp.exp(v - top) for v in sc]
    tot = functools.reduce(jnp.add, ex)
    probs = [(v / tot).astype(BF16).astype(F32) for v in ex]
    self_prob = functools.reduce(jnp.add, [jnp.where(pos == j, probs[j], 0.0) for j in range(n_slots)])
    for j in range(n_slots):
        p_ref[j] = jnp.where(pos == j, 0.0, probs[j])
    p_ref[n_slots] = self_prob
    c_v.wait()
    for h in range(n_heads):
        acc = p_ref[n_slots, h:h + 1, :] * qin[h // hx, 2, h % hx].astype(F32)
        for j in range(n_slots):
            acc = acc + p_ref[j, h:h + 1, :] * vc[h, j].astype(F32)
        o_t[h * hd:(h + 1) * hd, :] = acc
    oall[x] = o_t[...].T.astype(BF16)
    i_o = {i: new() for i in xs}
    for i in xs:
        send(oall.at[x], oall.at[x], dev(xp(i), c, y), i_o[i])
    for i in xs:
        send(wup_ref.at[:, xlane(fx, xp(i))], wup.at[w], dev(xp(i), c, y), i_ux[i])
    c_wo.wait()
    arrived(wo_land.at[1 - c], i_wo)
    wo[...] = jnp.concatenate([wo_land[0], wo_land[1]], axis=1)
    for i in xs:
        arrived(oall.at[lax.rem(x + nx - i, nx)], i_o[i])
    for g in range(nx):
        part = dot(oall[g], wo[...], NN).astype(BF16)
        for k in range(ny):
            st1[k, g * qr:(g + 1) * qr, :] = part[k * qr:(k + 1) * qr]
    i_r1 = {i: new() for i in ys}
    for i in ys:
        send(st1.at[yp(i)], in1.at[y], dev(x, c, yp(i)), i_r1[i])
    in1[y] = st1[y]
    c_gm.wait()
    arrived(gmx.at[1 - c], i_gm)
    gain_m = jnp.concatenate([gmx[0], gmx[1]], axis=1)
    for i in ys:
        arrived(in1.at[lax.rem(y + ny - i, ny)], i_r1[i])
    acc = in1[0].astype(F32)
    for k in range(1, ny):
        acc = acc + in1[k].astype(F32)
    for g in range(nx):
        hbuf[g * qr:(g + 1) * qr, :] = xall[g, qrow(y), xlane(dx, x)].astype(F32) + acc[g * qr:(g + 1) * qr]
    h = hbuf[...]
    sq = jnp.sum(h * h, axis=1, keepdims=True)
    sq = jnp.broadcast_to(sq, (rows, rows)).T[:8]
    st_s[...] = sq
    st_r[x] = sq
    i_s = {i: new() for i in xs}
    for i in xs:
        send(st_s, st_r.at[x], dev(xp(i), c, y), i_s[i])
    for i in xs:
        arrived(st_r.at[lax.rem(x + nx - i, nx)], i_s[i])
    tot = st_r[0]
    for j in range(1, nx):
        tot = tot + st_r[j]
    rstd = lax.rsqrt(tot * (1.0 / d_model) + NORM_EPS)
    rstd = jnp.broadcast_to(rstd[0:1], (rows, rows)).T[:, 0:1]
    mall[y, :, xlane(dx, x)] = (hbuf[...] * rstd * gain_m).astype(BF16)
    half = rows // 2
    lo, hi = pl.ds(0, half), pl.ds(half, half)

    def mpiece(yy, xx, part):
        return mall.at[yy, part, xlane(dx, xx)]

    i_m = {(p, a): new() for p in "xy" for a in range(1, 4)}
    i_mf = {(p, a, b): new() for p in "xy" for a in range(4) for b in range(1, 4)}
    for i in xs:
        send(mpiece(y, x, lo), mpiece(y, x, lo), dev(xp(i), c, y), i_m["x", i])
    for i in ys:
        send(mpiece(y, x, hi), mpiece(y, x, hi), dev(x, c, yp(i)), i_m["y", i])
    for k in ys:
        send(mpiece(y, x, lo), mpiece(y, x, lo), dev(x, c, yp(k)), i_mf["x", 0, k])
    for k in xs:
        send(mpiece(y, x, hi), mpiece(y, x, hi), dev(xp(k), c, y), i_mf["y", 0, k])
    for i in range(1, 4):
        a = lax.rem(x + nx - i, nx)
        arrived(mpiece(y, a, lo), i_m["x", i])
        for k in ys:
            send(mpiece(y, a, lo), mpiece(y, a, lo), dev(x, c, yp(k)), i_mf["x", i, k])
        b = lax.rem(y + ny - i, ny)
        arrived(mpiece(b, x, hi), i_m["y", i])
        for k in xs:
            send(mpiece(b, x, hi), mpiece(b, x, hi), dev(xp(k), c, y), i_mf["y", i, k])
    for i in xs:
        blk = wup.at[2 * lax.rem(x + nx - i, nx) + c]
        arrived(blk, i_ux[i])
        send(blk, blk, sib, i_us[i])
    for i in range(4):
        for k in range(1, 4):
            arrived(mpiece(lax.rem(y + ny - k, ny), lax.rem(x + nx - i, nx), lo), i_mf["x", i, k])
            arrived(mpiece(lax.rem(y + ny - i, ny), lax.rem(x + nx - k, nx), hi), i_mf["y", i, k])
    c_up.wait()
    for i in range(nx):
        arrived(wup.at[2 * lax.rem(x + nx - i, nx) + 1 - c], i_us[i])
    up = wup[...].reshape(d_model, fx)
    i_z = {(k, i): new() for k in range(ny) for i in xs}
    order = [lax.rem(y + 1 + k, ny) for k in range(ny)]
    for k, q in enumerate(order):
        z = dot(mall[q], up, NN)
        zall[q, :, xlane(fx, x)] = jax.nn.gelu(z, approximate=True).astype(BF16)
        for i in xs:
            send(zall.at[q, :, xlane(fx, x)], zall.at[q, :, xlane(fx, x)], dev(xp(i), c, y), i_z[k, i])
    c_dn.wait()
    arrived(wdn.at[1 - c], i_dn)
    dn = wdn[...].reshape(dx, zall.shape[2])
    i_r2 = {k: new() for k in ys}
    for k, q in enumerate(order):
        for i in xs:
            arrived(zall.at[q, :, xlane(fx, lax.rem(x + nx - i, nx))], i_z[k, i])
        part = dot(zall[q], dn, NT).astype(BF16)
        if k < ny - 1:
            st2[k] = part
            send(st2.at[k], in2.at[y], dev(x, c, q), i_r2[k + 1])
        else:
            in2[y] = part
    for i in ys:
        arrived(in2.at[lax.rem(y + ny - i, ny)], i_r2[i])
    acc = in2[0].astype(F32)
    for k in range(1, ny):
        acc = acc + in2[k].astype(F32)
    yst[...] = (hbuf[...] + acc).astype(BF16).reshape(nx, qr, dx)
    i_yx = {i: new() for i in xs}
    for i in xs:
        send(yst.at[xp(i)], yfull.at[y, :, xlane(dx, x)], dev(xp(i), c, y), i_yx[i])
    yfull[y, :, xlane(dx, x)] = yst[x]
    i_yy = {(i, k): new() for i in range(nx) for k in ys}
    for i in range(nx):
        blk = yfull.at[y, :, xlane(dx, lax.rem(x + nx - i, nx))]
        if i:
            arrived(blk, i_yx[i])
        for k in ys:
            send(blk, blk, dev(x, c, yp(k)), i_yy[i, k])
    for i in range(nx):
        for k in ys:
            arrived(yfull.at[lax.rem(y + ny - k, ny), :, xlane(dx, lax.rem(x + nx - i, nx))], i_yy[i, k])
    outs.append(local(yfull, y_ref))
    for cp in pending:
        cp.wait_send()
    for cp in outs:
        cp.wait()
    assert counter[0] <= N_REMOTE and counter[1] <= N_LOCAL


def solution(mesh):
    nx, ny = mesh.shape["wg"] // 2, mesh.shape["tp"]
    tok_axes = ("dp", "wg")
    in_specs = (P(tok_axes, None), P("wg"), P("wg"), P("wg", None, "tp", None), P("wg", "tp", None), P("tp", None, "wg"), P("wg", "tp"), P("tp", "wg"), P("tp", None), P("tp", None), P(None, None), P(tok_axes, "tp", None, None), P(tok_axes, "tp", None, None), P(tok_axes))
    out_specs = (P(tok_axes, None), P(tok_axes, "tp", None), P(tok_axes, "tp", None))

    def device_step(tokens, gain_attn, gain_mlp, w_qkv, w_rel, w_out, w_up, w_down, bias_u, bias_v, rel_table, k_cache, v_cache, positions):
        rows, d_model = tokens.shape
        ds = gain_attn.shape[0]
        dx = 2 * ds
        _, n_heads, n_slots, hd = k_cache.shape
        hx = n_heads // nx
        hw = n_heads * hd
        ff = w_up.shape[1]
        fx = ff // nx
        qr = rows // ny
        any_spec = pl.BlockSpec(memory_space=pl.ANY)
        vmem_spec = pl.BlockSpec(memory_space=pltpu.VMEM)
        vm = pltpu.VMEM
        scratch = [
            vm((nx, rows, d_model), BF16),
            vm((nx, rows, d_model), BF16),
            vm((2 * nx, 1, ds), F32),
            vm((2, 1, ds), F32),
            vm((2 * nx, 3, hx, hd, ds), BF16),
            vm((3 * hx * hd, d_model), BF16),
            vm((nx, 3, hx, hd, rows), BF16),
            vm((nx, 3, hx, hd, rows), BF16),
            vm((n_heads, n_slots, hd, rows), BF16),
            vm((n_heads, n_slots, hd, rows), BF16),
            vm((hw, ds), BF16),
            vm((n_slots, hw), F32),
            vm((2 * nx, n_slots, hw), F32),
            vm((n_slots, n_heads, rows), F32),
            vm((n_slots + 1, n_heads, rows), F32),
            vm((hw, rows), F32),
            vm((nx, rows, hw), BF16),
            vm((2, hw, ds), BF16),
            vm((hw, dx), BF16),
            vm((ny, rows, dx), BF16),
            vm((ny, rows, dx), BF16),
            vm((rows, dx), F32),
            vm((8, rows), F32),
            vm((nx, 8, rows), F32),
            vm((ny, rows, d_model), BF16),
            vm((2 * nx, ds, fx), BF16),
            vm((ny, rows, ff), BF16),
            vm((2, ds, ff), BF16),
            vm((ny - 1, rows, dx), BF16),
            vm((ny, rows, dx), BF16),
            vm((nx, qr, dx), BF16),
            vm((ny, qr, d_model), BF16),
            pltpu.SemaphoreType.DMA((N_REMOTE,)),
            pltpu.SemaphoreType.DMA((N_REMOTE,)),
            pltpu.SemaphoreType.DMA((N_LOCAL,)),
        ]
        y, kn, vn = pl.pallas_call(
            functools.partial(layer_kernel, nx, ny),
            out_shape=(
                jax.ShapeDtypeStruct((ny, qr, d_model), BF16),
                jax.ShapeDtypeStruct((n_heads, hd, rows), BF16),
                jax.ShapeDtypeStruct((n_heads, hd, rows), BF16),
            ),
            in_specs=[any_spec, vmem_spec, vmem_spec, any_spec, any_spec, any_spec, any_spec, any_spec, vmem_spec, vmem_spec, vmem_spec, any_spec, any_spec, vmem_spec],
            out_specs=(any_spec, any_spec, any_spec),
            scratch_shapes=scratch,
            compiler_params=pltpu.CompilerParams(collective_id=0, has_side_effects=True, vmem_limit_bytes=60 * 2**20),
        )(
            tokens, gain_attn[None, :], gain_mlp[None, :], w_qkv.transpose(1, 2, 3, 0), w_rel.transpose(1, 2, 0).reshape(hw, ds), w_out.reshape(hw, ds),
            w_up, w_down.T, bias_u, bias_v, rel_table, k_cache.transpose(1, 2, 3, 0), v_cache.transpose(1, 2, 3, 0), positions[None, :],
        )
        return y.reshape(rows, d_model), kn.transpose(2, 0, 1), vn.transpose(2, 0, 1)

    return jax.shard_map(device_step, mesh=mesh, in_specs=in_specs, out_specs=out_specs, check_vma=False)
```

```python
import functools
import math

import jax
import jax.numpy as jnp
from jax import lax
from jax.experimental import pallas as pl
from jax.experimental.pallas import tpu as pltpu
from jax.sharding import PartitionSpec as P

MESH = pl.DeviceIdType.MESH
NORM_EPS = 1e-6
BF16 = jnp.bfloat16
F32 = jnp.float32
NT = (((1,), (1,)), ((), ()))
NN = (((1,), (0,)), ((), ()))
N_REMOTE = 224
N_LOCAL = 32
UP_PARTS = (0, 96, 128, 272, 320)


def dot(a, b, dims):
    return lax.dot_general(a, b, dims, preferred_element_type=F32)


def layer_kernel(nx, ny, tok_ref, ga_ref, gm_ref, wqkv_ref, wrel_ref, wout_ref, wup_ref, wdn_ref, bu_ref, bv_ref, relt_ref, kc_ref, vc_ref, pos_ref,
                 y_ref, kn_ref, vn_ref,
                 xall, nall, gst, gall, gain, wq_land, wpk, wq, qst, qin, kc, vc, wrel, rsend, rsib, rland, rfull, rel_diag, s_ref, p_ref, o_t, oall, wo_land, wo,
                 st1, in1, hbuf, st_s, st_r, mall, wup, zall, wdn, st2, in2, yst, yfull,
                 ss, rs, ls):
    w = lax.axis_index("wg")
    x, c, y = w // 2, w % 2, lax.axis_index("tp")
    rows, d_model = tok_ref.shape
    ds = ga_ref.shape[0]
    dx = 2 * ds
    n_heads, n_slots, hd, _ = kc_ref.shape
    hx = n_heads // nx
    fx = wup_ref.shape[1] // nx
    qr = rows // ny
    hw = n_heads * hd
    ff = wup_ref.shape[1]

    def dev(xx, cc, yy):
        return {"wg": 2 * xx + cc, "tp": yy}

    def xp(i):
        return lax.rem(x + i, nx)

    def yp(i):
        return lax.rem(y + i, ny)

    sib = dev(x, 1 - c, y)
    right, left = dev(xp(1), c, y), dev(xp(nx - 1), c, y)
    above, below = dev(x, c, yp(1)), dev(x, c, yp(ny - 1))
    xof = {"S": x, "L": xp(nx - 1), "R": xp(1), "O": xp(2)}
    yof = {"S": y, "D": yp(ny - 1), "U": yp(1), "O": yp(2)}
    ids = {}
    pending = []
    n_local = [0]

    def nid(key):
        return ids.setdefault(key, len(ids))

    def send(src, dst, to, key):
        i = nid(key)
        cp = pltpu.make_async_remote_copy(src_ref=src, dst_ref=dst, send_sem=ss.at[i], recv_sem=rs.at[i], device_id=to, device_id_type=MESH)
        cp.start()
        pending.append(cp)

    def arrived(dst, key):
        i = nid(key)
        pltpu.make_async_remote_copy(src_ref=dst, dst_ref=dst, send_sem=ss.at[i], recv_sem=rs.at[i], device_id=sib, device_id_type=MESH).wait_recv()

    def local(src, dst):
        cp = pltpu.make_async_copy(src, dst, ls.at[n_local[0]])
        n_local[0] += 1
        cp.start()
        return cp

    def lanes(size, k):
        return pl.ds(pl.multiple_of(k * size, 128), size)

    def rowsl(start, size):
        return pl.ds(pl.multiple_of(start, 16), size)

    def x_start(name, unit, own=None):
        own = own or (lambda h: unit(x, h))
        for h, to, frm in ((0, right, "L"), (1, left, "R"), (1, right, "L"), (0, left, "R")):
            send(own(h), unit(x, h), to, (name, frm, h))

    def x_relay(name, unit, frm):
        h, to = (0, right) if frm == "L" else (1, left)
        arrived(unit(xof[frm], h), (name, frm, h))
        send(unit(xof[frm], h), unit(xof[frm], h), to, (name, "O", h))

    def x_wait(name, unit, frm, h):
        arrived(unit(xof[frm], h), (name, frm, h))

    def y_send(name, unit, px, h):
        blk = unit(xof[px], y, h)
        send(blk, blk, above, (name, px, "D", h))
        send(blk, blk, below, (name, px, "U", h))

    def y_relay(name, unit, px, frm):
        h, to = (0, above) if frm == "D" else (1, below)
        blk = unit(xof[px], yof[frm], h)
        arrived(blk, (name, px, frm, h))
        send(blk, blk, to, (name, px, "O", h))

    def y_wait(name, unit, px, frm, h):
        arrived(unit(xof[px], yof[frm], h), (name, px, frm, h))

    c_wq = local(wqkv_ref.at[:, :, c], wq_land.at[c])
    c_rel = local(wrel_ref, wrel)
    c_x = local(tok_ref, xall.at[x])
    c_k = local(kc_ref, kc)
    c_v = local(vc_ref, vc)
    c_wo = local(wout_ref, wo_land.at[c])
    c_up = local(wup_ref.at[:, lanes(fx, x)], wup.at[w])
    c_dn = local(wdn_ref, wdn.at[c])
    gst[0:1, :] = ga_ref[...].reshape(1, ds)
    gst[1:2, :] = gm_ref[...].reshape(1, ds)
    gall[w] = gst[...]

    barrier = pltpu.get_barrier_semaphore()
    peers = [dev(xp(i), c, y) for i in range(1, nx)] + [dev(x, c, yp(i)) for i in range(1, ny)] + [sib]
    for peer in peers:
        pl.semaphore_signal(barrier, inc=1, device_id=peer, device_id_type=MESH)
    pl.semaphore_wait(barrier, len(peers))

    hq = qr // 2

    def tok_unit(xx, yy, h):
        return xall.at[xx, rowsl(yy * qr + h * hq, hq)]

    def tok_x(xx, h):
        return tok_unit(xx, y, h)

    x_start("tx", tok_x, lambda h: tok_ref.at[rowsl(y * qr + h * hq, hq)])
    send(wqkv_ref.at[:, :, 1 - c], wq_land.at[c], sib, "wqs")
    send(gst, gall.at[w], sib, ("g", 0))
    for i in range(1, nx):
        send(gst, gall.at[w], dev(xp(i), c, y), ("g", i))
    c_rel.wait()
    tab = relt_ref[:, lanes(dx, x)]
    tab = jnp.where(c == 0, tab[:, :ds], tab[:, ds:])
    part = dot(tab, wrel[...], NT)
    hs = n_slots // 2
    rsend[...] = part.reshape(2, hs, hw)
    send(rsend.at[1 - c], rsib, sib, "r0")
    x_relay("tx", tok_x, "L")
    y_send("ty", tok_unit, "L", 0)
    x_relay("tx", tok_x, "R")
    y_send("ty", tok_unit, "R", 1)
    c_wq.wait()
    arrived(wq_land.at[1 - c], "wqs")
    for s in range(3):
        for j in range(nx):
            wpk[s, j] = jnp.concatenate([wq_land[0, s, j], wq_land[1, s, j]], axis=1)
    for i, key in ((1, "L"), (nx - 1, "R"), (2, "O")):
        send(wpk.at[:, xp(i)], wq.at[:, c, :, lanes(dx, x)], dev(xp(i), c, y), ("wx", key))
    wq[:, c, :, lanes(dx, x)] = wpk[:, x]
    send(wpk.at[:, x], wq.at[:, c, :, lanes(dx, x)], sib, ("ws", "S"))
    arrived(rsib, "r0")
    rland[x] = rsend[c] + rsib[...]
    for i, key in ((1, "L"), (nx - 1, "R"), (2, "O")):
        send(rland.at[x], rland.at[x], dev(xp(i), c, y), ("r1", key))
    for frm, h in (("L", 1), ("R", 0), ("O", 0), ("O", 1)):
        x_wait("tx", tok_x, frm, h)
        y_send("ty", tok_unit, frm, h)

    def up_send(p):
        r0, r1 = UP_PARTS[p], UP_PARTS[p + 1]
        for i, key in ((1, "L"), (nx - 1, "R"), (2, "O")):
            send(wup_ref.at[r0:r1, lanes(fx, xp(i))], wup.at[w, r0:r1], dev(xp(i), c, y), ("ux", p, key))

    def up_relay(p):
        r0, r1 = UP_PARTS[p], UP_PARTS[p + 1]
        for key in "LRO":
            blk = wup.at[2 * xof[key] + c, r0:r1]
            arrived(blk, ("ux", p, key))
            send(blk, blk, sib, ("us", p, key))

    up_send(0)
    send(wout_ref, wo_land.at[c], sib, "wo")
    send(wdn_ref, wdn.at[c], sib, "dn")
    send(wup_ref.at[:, lanes(fx, x)], wup.at[w], sib, "uown")
    for i in range(1, nx):
        blk = gall.at[2 * lax.rem(x + nx - i, nx) + c]
        arrived(blk, ("g", i))
        send(blk, blk, sib, ("gs", i))
    arrived(gall.at[2 * x + 1 - c], ("g", 0))
    for i in range(1, nx):
        arrived(gall.at[2 * lax.rem(x + nx - i, nx) + 1 - c], ("gs", i))
    gain[...] = jnp.concatenate([gall[j, 0:1, :] for j in range(2 * nx)], axis=1)
    blk_rows = 32

    def norm_group(g):
        def norm_block(r, carry):
            b = pl.ds(pl.multiple_of(r * blk_rows, blk_rows), blk_rows)
            v = xall[g, b, :].astype(F32)
            ms = jnp.mean(v * v, axis=-1, keepdims=True)
            nall[g, b, :] = (v * lax.rsqrt(ms + NORM_EPS) * gain[...]).astype(BF16)
            return carry

        lax.fori_loop(0, rows // blk_rows, norm_block, 0)

    c_x.wait()
    norm_group(x)
    for px, frm in (("L", "D"), ("R", "U"), ("L", "U"), ("R", "D"), ("O", "D"), ("O", "U")):
        y_relay("ty", tok_unit, px, frm)
    for key in "LRO":
        blk = wq.at[:, c, :, lanes(dx, xof[key])]
        arrived(blk, ("wx", key))
        send(blk, blk, sib, ("ws", key))
    for px in "LRO":
        for frm, h in (("D", 1), ("U", 0), ("O", 0), ("O", 1)):
            y_wait("ty", tok_unit, px, frm, h)
        norm_group(xof[px])
    for key in "SLRO":
        arrived(wq.at[:, 1 - c, :, lanes(dx, xof[key])], ("ws", key))
    wqv = wq[...].reshape(3 * hx * hd, d_model)
    for i, key in ((2, "O"), (1, "L"), (nx - 1, "R"), (0, "S")):
        g = xp(i)
        res = dot(wqv, nall[g], NT).astype(BF16).reshape(3, hx, hd, rows)
        if i:
            qst[i - 1] = res
            send(qst.at[i - 1], qin.at[x], dev(g, c, y), ("q", key))
        else:
            qin[x] = res
    up_send(1)
    for key in "LRO":
        arrived(rland.at[xof[key]], ("r1", key))
    rel = rland[0]
    for j in range(1, nx):
        rel = rel + rland[j]
    rfull[c] = rel
    send(rfull.at[c], rfull.at[c], sib, "r2")
    up_relay(0)
    arrived(rfull.at[1 - c], "r2")
    rel = rfull[...].reshape(n_slots, hw).astype(BF16).astype(F32)
    rel = jnp.broadcast_to(rel[:, None, :], (n_slots, n_heads, hw)).reshape(n_slots * n_heads, hw)
    col = lax.broadcasted_iota(jnp.int32, rel.shape, 1)
    row_head = lax.rem(lax.broadcasted_iota(jnp.int32, rel.shape, 0), n_heads)
    keep = (col >= row_head * hd) & (col < row_head * hd + hd)
    rel_diag[...] = jnp.where(keep, rel, 0.0).astype(BF16)
    c_k.wait()
    for key in "LRO":
        arrived(qin.at[xof[key]], ("q", key))
    outs = []
    for j in range(nx):
        outs.append(local(qin.at[j, 1], kn_ref.at[j * hx:(j + 1) * hx]))
        outs.append(local(qin.at[j, 2], vn_ref.at[j * hx:(j + 1) * hx]))
    pos = pos_ref[...]
    bu_t, bv_t = bu_ref[...].T, bv_ref[...].T
    scale = 1.0 / math.sqrt(hd)
    selfs, qvs = [], []
    for h in range(n_heads):
        q = qin[h // hx, 0, h % hx].astype(F32)
        qu = (q + bu_t[:, h:h + 1]).astype(BF16).astype(F32)
        qvs.append((q + bv_t[:, h:h + 1]).astype(BF16))
        selfs.append(jnp.sum(qu * qin[h // hx, 1, h % hx].astype(F32), axis=0, keepdims=True))
        for j in range(n_slots):
            s_ref[j, h:h + 1, :] = jnp.sum(kc[h, j].astype(F32) * qu, axis=0, keepdims=True)
    self_score = jnp.concatenate(selfs, axis=0)
    rel_all = dot(rel_diag[...], jnp.concatenate(qvs, axis=0), NN)
    rel_all = [rel_all[r * n_heads:(r + 1) * n_heads] for r in range(n_slots)][::-1]
    shift = n_slots - 1 - pos
    bit = 1
    while bit < n_slots:
        take = (shift // bit) % 2 == 1
        rel_all = [jnp.where(take, rel_all[j + bit], rel_all[j]) if j + bit < n_slots else rel_all[j] for j in range(n_slots)]
        bit *= 2
    sc = []
    for j in range(n_slots):
        content = jnp.where(pos == j, self_score, s_ref[j])
        sc.append(jnp.where(pos >= j, (content + rel_all[j]) * scale, -1e30))
    top = functools.reduce(jnp.maximum, sc)
    ex = [jnp.exp(v - top) for v in sc]
    tot = functools.reduce(jnp.add, ex)
    probs = [(v / tot).astype(BF16).astype(F32) for v in ex]
    self_prob = functools.reduce(jnp.add, [jnp.where(pos == j, probs[j], 0.0) for j in range(n_slots)])
    for j in range(n_slots):
        p_ref[j] = jnp.where(pos == j, 0.0, probs[j])
    p_ref[n_slots] = self_prob
    c_v.wait()
    for h in range(n_heads):
        acc = p_ref[n_slots, h:h + 1, :] * qin[h // hx, 2, h % hx].astype(F32)
        for j in range(n_slots):
            acc = acc + p_ref[j, h:h + 1, :] * vc[h, j].astype(F32)
        o_t[h * hd:(h + 1) * hd, :] = acc
    oall[x] = o_t[...].T.astype(BF16)
    half = rows // 2

    def o_unit(xx, h):
        return oall.at[xx, h * half:(h + 1) * half]

    x_start("o", o_unit)
    up_relay(1)
    c_wo.wait()
    arrived(wo_land.at[1 - c], "wo")
    wo[...] = jnp.concatenate([wo_land[0], wo_land[1]], axis=1)

    def out_proj(px):
        g = xof[px]
        part = dot(oall[g], wo[...], NN).astype(BF16)
        st1[g] = part.reshape(ny, qr, dx)
        for i, key in ((2, "O"), (1, "D"), (ny - 1, "U")):
            send(st1.at[g, yp(i)], in1.at[y, g], dev(x, c, yp(i)), ("r1y", px, key))
        in1[y, g] = st1[g, y]

    x_relay("o", o_unit, "L")
    x_relay("o", o_unit, "R")
    up_send(2)
    out_proj("S")
    x_wait("o", o_unit, "L", 1)
    out_proj("L")
    x_wait("o", o_unit, "R", 0)
    out_proj("R")
    x_wait("o", o_unit, "O", 0)
    x_wait("o", o_unit, "O", 1)
    out_proj("O")
    gain_m = jnp.concatenate([gall[2 * x, 1:2, :], gall[2 * x + 1, 1:2, :]], axis=1)
    for px in "SLRO":
        for key in "DUO":
            arrived(in1.at[yof[key], xof[px]], ("r1y", px, key))
    for g in range(nx):
        acc = in1[0, g].astype(F32)
        for k in range(1, ny):
            acc = acc + in1[k, g].astype(F32)
        hbuf[g * qr:(g + 1) * qr, :] = xall[g, rowsl(y * qr, qr), lanes(dx, x)].astype(F32) + acc
    h = hbuf[...]
    sq = jnp.sum(h * h, axis=1, keepdims=True)
    sq = jnp.broadcast_to(sq, (rows, rows)).T[:8]
    st_s[...] = sq
    st_r[x] = sq
    for i, key in ((2, "O"), (1, "L"), (nx - 1, "R")):
        send(st_s, st_r.at[x], dev(xp(i), c, y), ("st", key))
    up_send(3)
    for key in "LRO":
        arrived(st_r.at[xof[key]], ("st", key))
    tot = st_r[0]
    for j in range(1, nx):
        tot = tot + st_r[j]
    rstd = lax.rsqrt(tot * (1.0 / d_model) + NORM_EPS)
    rstd = jnp.broadcast_to(rstd[0:1], (rows, rows)).T[:, 0:1]
    mall[y, :, lanes(dx, x)] = (hbuf[...] * rstd * gain_m).astype(BF16)

    def m_unit(xx, yy, h):
        return mall.at[yy, h * half:(h + 1) * half, lanes(dx, xx)]

    def m_x(xx, h):
        return m_unit(xx, y, h)

    x_start("mx", m_x)
    y_send("my", m_unit, "S", 0)
    y_send("my", m_unit, "S", 1)
    x_relay("mx", m_x, "L")
    y_send("my", m_unit, "L", 0)
    x_relay("mx", m_x, "R")
    y_send("my", m_unit, "R", 1)
    up_relay(2)
    for frm, h in (("L", 1), ("R", 0), ("O", 0), ("O", 1)):
        x_wait("mx", m_x, frm, h)
        y_send("my", m_unit, frm, h)
    up_relay(3)
    c_up.wait()
    arrived(wup.at[2 * x + 1 - c], "uown")
    for p in range(4):
        for key in "LRO":
            arrived(wup.at[2 * xof[key] + 1 - c, UP_PARTS[p]:UP_PARTS[p + 1]], ("us", p, key))

    def z_unit(py):
        return lambda xx, h: zall.at[yof[py], h * half:(h + 1) * half, lanes(fx, xx)]

    def hidden(py):
        z = dot(mall[yof[py]], wup[...].reshape(d_model, fx), NN)
        zall[yof[py], :, lanes(fx, x)] = jax.nn.gelu(z, approximate=True).astype(BF16)
        x_start(("z", py), z_unit(py))

    def z_relay(py):
        x_relay(("z", py), z_unit(py), "L")
        x_relay(("z", py), z_unit(py), "R")

    def down(py):
        for frm, h in (("L", 1), ("R", 0), ("O", 0), ("O", 1)):
            x_wait(("z", py), z_unit(py), frm, h)
        part = dot(zall[yof[py]], wdn[...].reshape(dx, ff), NT).astype(BF16)
        if py == "S":
            in2[y] = part
        else:
            k = "DUO".index(py)
            st2[k] = part
            send(st2.at[k], in2.at[y], dev(x, c, yof[py]), ("r2y", {"D": "U", "U": "D", "O": "O"}[py]))

    hidden("S")
    z_relay("S")
    for px in "SLRO":
        y_relay("my", m_unit, px, "D")
        y_relay("my", m_unit, px, "U")
    for px in "SLRO":
        y_wait("my", m_unit, px, "D", 1)
    hidden("D")
    for px in "SLRO":
        y_wait("my", m_unit, px, "U", 0)
    hidden("U")
    c_dn.wait()
    arrived(wdn.at[1 - c], "dn")
    z_relay("D")
    down("S")
    z_relay("U")
    for px in "SLRO":
        y_wait("my", m_unit, px, "O", 0)
        y_wait("my", m_unit, px, "O", 1)
    hidden("O")
    down("D")
    z_relay("O")
    down("U")
    down("O")
    for key in "DUO":
        arrived(in2.at[yof[key]], ("r2y", key))
    acc = in2[0].astype(F32)
    for k in range(1, ny):
        acc = acc + in2[k].astype(F32)
    yst[...] = (hbuf[...] + acc).astype(BF16).reshape(nx, qr, dx)
    for i, key in ((2, "O"), (1, "L"), (nx - 1, "R")):
        send(yst.at[xp(i)], yfull.at[y, :, lanes(dx, x)], dev(xp(i), c, y), ("yx", key))
    yfull[y, :, lanes(dx, x)] = yst[x]
    for px in "SLRO":
        blk = yfull.at[y, :, lanes(dx, xof[px])]
        if px != "S":
            arrived(blk, ("yx", px))
        for i, key in ((1, "D"), (ny - 1, "U"), (2, "O")):
            send(blk, blk, dev(x, c, yp(i)), ("yy", px, key))
    for px in "SLRO":
        for key in "DUO":
            arrived(yfull.at[yof[key], :, lanes(dx, xof[px])], ("yy", px, key))
    outs.append(local(yfull, y_ref))
    for cp in pending:
        cp.wait_send()
    for cp in outs:
        cp.wait()
    assert len(ids) <= N_REMOTE and n_local[0] <= N_LOCAL


def solution(mesh):
    nx, ny = mesh.shape["wg"] // 2, mesh.shape["tp"]
    tok_axes = ("dp", "wg")
    in_specs = (P(tok_axes, None), P("wg"), P("wg"), P("wg", None, "tp", None), P("wg", "tp", None), P("tp", None, "wg"), P("wg", "tp"), P("tp", "wg"), P("tp", None), P("tp", None), P(None, None), P(tok_axes, "tp", None, None), P(tok_axes, "tp", None, None), P(tok_axes))
    out_specs = (P(tok_axes, None), P(tok_axes, "tp", None), P(tok_axes, "tp", None))

    def device_step(tokens, gain_attn, gain_mlp, w_qkv, w_rel, w_out, w_up, w_down, bias_u, bias_v, rel_table, k_cache, v_cache, positions):
        rows, d_model = tokens.shape
        ds = gain_attn.shape[0]
        dx = 2 * ds
        _, n_heads, n_slots, hd = k_cache.shape
        hx = n_heads // nx
        hw = n_heads * hd
        ff = w_up.shape[1]
        fx = ff // nx
        qr = rows // ny
        any_spec = pl.BlockSpec(memory_space=pl.ANY)
        vmem_spec = pl.BlockSpec(memory_space=pltpu.VMEM)
        vm = pltpu.VMEM
        scratch = [
            vm((nx, rows, d_model), BF16),
            vm((nx, rows, d_model), BF16),
            vm((2, ds), F32),
            vm((2 * nx, 2, ds), F32),
            vm((1, d_model), F32),
            vm((2, 3, nx, hd, ds), BF16),
            vm((3, nx, hd, dx), BF16),
            vm((3, hx, hd, d_model), BF16),
            vm((nx - 1, 3, hx, hd, rows), BF16),
            vm((nx, 3, hx, hd, rows), BF16),
            vm((n_heads, n_slots, hd, rows), BF16),
            vm((n_heads, n_slots, hd, rows), BF16),
            vm((hw, ds), BF16),
            vm((2, n_slots // 2, hw), F32),
            vm((n_slots // 2, hw), F32),
            vm((nx, n_slots // 2, hw), F32),
            vm((2, n_slots // 2, hw), F32),
            vm((n_slots * n_heads, hw), BF16),
            vm((n_slots, n_heads, rows), F32),
            vm((n_slots + 1, n_heads, rows), F32),
            vm((hw, rows), F32),
            vm((nx, rows, hw), BF16),
            vm((2, hw, ds), BF16),
            vm((hw, dx), BF16),
            vm((nx, ny, qr, dx), BF16),
            vm((ny, nx, qr, dx), BF16),
            vm((rows, dx), F32),
            vm((8, rows), F32),
            vm((nx, 8, rows), F32),
            vm((ny, rows, d_model), BF16),
            vm((2 * nx, ds, fx), BF16),
            vm((ny, rows, ff), BF16),
            vm((2, ds, ff), BF16),
            vm((ny - 1, rows, dx), BF16),
            vm((ny, rows, dx), BF16),
            vm((nx, qr, dx), BF16),
            vm((ny, qr, d_model), BF16),
            pltpu.SemaphoreType.DMA((N_REMOTE,)),
            pltpu.SemaphoreType.DMA((N_REMOTE,)),
            pltpu.SemaphoreType.DMA((N_LOCAL,)),
        ]
        y, kn, vn = pl.pallas_call(
            functools.partial(layer_kernel, nx, ny),
            out_shape=(
                jax.ShapeDtypeStruct((ny, qr, d_model), BF16),
                jax.ShapeDtypeStruct((n_heads, hd, rows), BF16),
                jax.ShapeDtypeStruct((n_heads, hd, rows), BF16),
            ),
            in_specs=[any_spec, vmem_spec, vmem_spec, any_spec, any_spec, any_spec, any_spec, any_spec, vmem_spec, vmem_spec, vmem_spec, any_spec, any_spec, vmem_spec],
            out_specs=(any_spec, any_spec, any_spec),
            scratch_shapes=scratch,
            compiler_params=pltpu.CompilerParams(collective_id=0, has_side_effects=True, vmem_limit_bytes=60 * 2**20),
        )(
            tokens, gain_attn, gain_mlp, w_qkv.transpose(1, 2, 3, 0).reshape(3, nx, hx, hd, ds), w_rel.transpose(1, 2, 0).reshape(hw, ds), w_out.reshape(hw, ds),
            w_up, w_down.T, bias_u, bias_v, rel_table, k_cache.transpose(1, 2, 3, 0), v_cache.transpose(1, 2, 3, 0), positions[None, :],
        )
        return y.reshape(rows, d_model), kn.transpose(2, 0, 1), vn.transpose(2, 0, 1)

    return jax.shard_map(device_step, mesh=mesh, in_specs=in_specs, out_specs=out_specs, check_vma=False)
```

```python
import functools
import math

import jax
import jax.numpy as jnp
from jax import lax
from jax.experimental import pallas as pl
from jax.experimental.pallas import tpu as pltpu
from jax.sharding import PartitionSpec as P

MESH = pl.DeviceIdType.MESH
NORM_EPS = 1e-6
BF16 = jnp.bfloat16
F32 = jnp.float32
NT = (((1,), (1,)), ((), ()))
NN = (((1,), (0,)), ((), ()))
N_REMOTE = 256
N_LOCAL = 32
UP_PARTS = (0, 64, 128, 272, 320)


def dot(a, b, dims):
    return lax.dot_general(a, b, dims, preferred_element_type=F32)


def layer_kernel(nx, ny, tok_ref, ga_ref, gm_ref, wqkv_ref, wrel_ref, wout_ref, wup_ref, wdn_ref, bu_ref, bv_ref, relt_ref, kc_ref, vc_ref, pos_ref,
                 y_ref, kn_ref, vn_ref,
                 xall, nall, qacc, gst, gall, gain, wq_land, wpk, wq, qst, qin, kc, vc, wrel, rsend, rsib, rland, rfull, rel_diag, s_ref, p_ref, o_t, oall, wo_land, wo,
                 st1, in1, hbuf, st_s, st_r, mall, wup, zall, wdn, st2, in2, yst, yfull,
                 ss, rs, ls):
    w = lax.axis_index("wg")
    x, c, y = w // 2, w % 2, lax.axis_index("tp")
    rows, d_model = tok_ref.shape
    ds = ga_ref.shape[0]
    dx = 2 * ds
    n_heads, n_slots, hd, _ = kc_ref.shape
    hx = n_heads // nx
    fx = wup_ref.shape[1] // nx
    qr = rows // ny
    hw = n_heads * hd
    ff = wup_ref.shape[1]

    def dev(xx, cc, yy):
        return {"wg": 2 * xx + cc, "tp": yy}

    def xp(i):
        return lax.rem(x + i, nx)

    def yp(i):
        return lax.rem(y + i, ny)

    sib = dev(x, 1 - c, y)
    right, left = dev(xp(1), c, y), dev(xp(nx - 1), c, y)
    above, below = dev(x, c, yp(1)), dev(x, c, yp(ny - 1))
    xof = {"S": x, "L": xp(nx - 1), "R": xp(1), "O": xp(2)}
    yof = {"S": y, "D": yp(ny - 1), "U": yp(1), "O": yp(2)}
    ids = {}
    pending = []
    n_local = [0]

    def nid(key):
        return ids.setdefault(key, len(ids))

    def send(src, dst, to, key):
        i = nid(key)
        cp = pltpu.make_async_remote_copy(src_ref=src, dst_ref=dst, send_sem=ss.at[i], recv_sem=rs.at[i], device_id=to, device_id_type=MESH)
        cp.start()
        pending.append(cp)

    def arrived(dst, key):
        i = nid(key)
        pltpu.make_async_remote_copy(src_ref=dst, dst_ref=dst, send_sem=ss.at[i], recv_sem=rs.at[i], device_id=sib, device_id_type=MESH).wait_recv()

    def local(src, dst):
        cp = pltpu.make_async_copy(src, dst, ls.at[n_local[0]])
        n_local[0] += 1
        cp.start()
        return cp

    def lanes(size, k):
        return pl.ds(pl.multiple_of(k * size, 128), size)

    def rowsl(start, size):
        return pl.ds(pl.multiple_of(start, 16), size)

    def x_start(name, unit):
        for h, to, frm in ((0, right, "L"), (1, left, "R"), (1, right, "L"), (0, left, "R")):
            send(unit(x, h), unit(x, h), to, (name, frm, h))

    def x_relay(name, unit, frm):
        h, to = (0, right) if frm == "L" else (1, left)
        arrived(unit(xof[frm], h), (name, frm, h))
        send(unit(xof[frm], h), unit(xof[frm], h), to, (name, "O", h))

    def x_wait(name, unit, frm, h):
        arrived(unit(xof[frm], h), (name, frm, h))

    def y_send(name, unit, px, h):
        blk = unit(xof[px], y, h)
        send(blk, blk, above, (name, px, "D", h))
        send(blk, blk, below, (name, px, "U", h))

    def y_relay(name, unit, px, frm):
        h, to = (0, above) if frm == "D" else (1, below)
        blk = unit(xof[px], yof[frm], h)
        arrived(blk, (name, px, frm, h))
        send(blk, blk, to, (name, px, "O", h))

    def y_wait(name, unit, px, frm, h):
        arrived(unit(xof[px], yof[frm], h), (name, px, frm, h))

    c_wq = local(wqkv_ref.at[:, :, c], wq_land.at[c])
    c_rel = local(wrel_ref, wrel)
    c_x = local(tok_ref, xall.at[x])
    c_k = local(kc_ref, kc)
    c_v = local(vc_ref, vc)
    c_wo = local(wout_ref, wo_land.at[c])
    c_up = local(wup_ref.at[:, lanes(fx, x)], wup.at[w])
    c_dn = local(wdn_ref, wdn.at[c])
    gst[0:1, :] = ga_ref[...].reshape(1, ds)
    gst[1:2, :] = gm_ref[...].reshape(1, ds)
    gall[w] = gst[...]

    barrier = pltpu.get_barrier_semaphore()
    peers = [dev(xp(i), c, y) for i in range(1, nx)] + [dev(x, c, yp(i)) for i in range(1, ny)] + [sib]
    for peer in peers:
        pl.semaphore_signal(barrier, inc=1, device_id=peer, device_id_type=MESH)
    pl.semaphore_wait(barrier, len(peers))

    hq = qr // 2

    def tok_unit(xx, yy, h):
        return xall.at[xx, rowsl(yy * qr + h * hq, hq)]

    def tok_x(xx, h):
        return tok_unit(xx, y, h)

    c_x.wait()
    x_start("tx", tok_x)
    send(wqkv_ref.at[:, :, 1 - c], wq_land.at[c], sib, "wqs")
    send(gst, gall.at[w], sib, ("g", 0))
    for i in range(1, nx):
        send(gst, gall.at[w], dev(xp(i), c, y), ("g", i))
    c_rel.wait()
    tab = relt_ref[:, lanes(dx, x)]
    tab = jnp.where(c == 0, tab[:, :ds], tab[:, ds:])
    part = dot(tab, wrel[...], NT)
    hs = n_slots // 2
    rsend[...] = part.reshape(2, hs, hw)
    send(rsend.at[1 - c], rsib, sib, "r0")
    x_relay("tx", tok_x, "L")
    y_send("ty", tok_unit, "L", 0)
    x_relay("tx", tok_x, "R")
    y_send("ty", tok_unit, "R", 1)
    c_wq.wait()
    arrived(wq_land.at[1 - c], "wqs")
    for s in range(3):
        for j in range(nx):
            wpk[j, s * hd:(s + 1) * hd, :] = jnp.concatenate([wq_land[0, s, j], wq_land[1, s, j]], axis=1)

    def wq_unit(cc, xx):
        return wq.at[rowsl(cc * (3 * hd), 3 * hd), lanes(dx, xx)]

    for i, key in ((1, "L"), (nx - 1, "R"), (2, "O")):
        send(wpk.at[xp(i)], wq_unit(c, x), dev(xp(i), c, y), ("wx", key))
    wq[rowsl(c * (3 * hd), 3 * hd), lanes(dx, x)] = wpk[x]
    send(wpk.at[x], wq_unit(c, x), sib, ("ws", "S"))
    arrived(rsib, "r0")
    rland[x] = rsend[c] + rsib[...]
    for i, key in ((1, "L"), (nx - 1, "R"), (2, "O")):
        send(rland.at[x], rland.at[x], dev(xp(i), c, y), ("r1", key))
    for frm, h in (("L", 1), ("R", 0), ("O", 0), ("O", 1)):
        x_wait("tx", tok_x, frm, h)
        y_send("ty", tok_unit, frm, h)

    def up_send(p):
        r0, r1 = UP_PARTS[p], UP_PARTS[p + 1]
        for i, key in ((1, "L"), (nx - 1, "R"), (2, "O")):
            send(wup_ref.at[r0:r1, lanes(fx, xp(i))], wup.at[w, r0:r1], dev(xp(i), c, y), ("ux", p, key))

    def up_relay(p):
        r0, r1 = UP_PARTS[p], UP_PARTS[p + 1]
        for key in "LRO":
            blk = wup.at[2 * xof[key] + c, r0:r1]
            arrived(blk, ("ux", p, key))
            send(blk, blk, sib, ("us", p, key))

    up_send(0)
    send(wout_ref, wo_land.at[c], sib, "wo")
    send(wdn_ref, wdn.at[c], sib, "dn")
    send(wup_ref.at[:, lanes(fx, x)], wup.at[w], sib, "uown")
    for i in range(1, nx):
        blk = gall.at[2 * lax.rem(x + nx - i, nx) + c]
        arrived(blk, ("g", i))
        send(blk, blk, sib, ("gs", i))
    arrived(gall.at[2 * x + 1 - c], ("g", 0))
    for i in range(1, nx):
        arrived(gall.at[2 * lax.rem(x + nx - i, nx) + 1 - c], ("gs", i))
    gain[...] = jnp.concatenate([gall[j, 0:1, :] for j in range(2 * nx)], axis=1)
    def norm_block(px, yy):
        v = xall[xof[px], rowsl(yy * qr, qr), :].astype(F32)
        ms = jnp.mean(v * v, axis=-1, keepdims=True)
        nall[rowsl("ORLS".index(px) * rows + yy * qr, qr), :] = (v * lax.rsqrt(ms + NORM_EPS) * gain[...]).astype(BF16)

    def norm_own(r, carry):
        norm_block("S", r)
        return carry

    lax.fori_loop(0, ny, norm_own, 0)
    for px in "LRO":
        norm_block(px, y)
    for px, frm in (("L", "D"), ("R", "U"), ("L", "U"), ("R", "D"), ("O", "D"), ("O", "U")):
        y_relay("ty", tok_unit, px, frm)
    for px in "LRO":
        y_wait("ty", tok_unit, px, "D", 1)
        norm_block(px, yof["D"])
        y_wait("ty", tok_unit, px, "U", 0)
        norm_block(px, yof["U"])
    def qkv_part(key, p):
        k = lanes(dx, xof[key])
        return dot(wq[:, k], nall[2 * p * rows:2 * (p + 1) * rows, k], NT)

    def wq_relay(key):
        arrived(wq_unit(c, xof[key]), ("wx", key))
        send(wq_unit(c, xof[key]), wq_unit(c, xof[key]), sib, ("ws", key))

    wq_relay("L")
    wq_relay("R")
    for px in "LRO":
        y_wait("ty", tok_unit, px, "O", 0)
        y_wait("ty", tok_unit, px, "O", 1)
        norm_block(px, yof["O"])
    wq_relay("O")
    arrived(wq_unit(1 - c, x), ("ws", "S"))
    for p in range(2):
        qacc[p] = qkv_part("S", p)
    for key in "LR":
        arrived(wq_unit(1 - c, xof[key]), ("ws", key))
    for p in range(2):
        qacc[p] += qkv_part("L", p) + qkv_part("R", p)
    arrived(wq_unit(1 - c, xof["O"]), ("ws", "O"))
    for p, pair in enumerate((((2, "O"), (1, "L")), ((nx - 1, "R"), (0, "S")))):
        res = (qacc[p] + qkv_part("O", p)).astype(BF16).reshape(hx, 3, hd, 2 * rows)
        for k, (i, key) in enumerate(pair):
            if i:
                qst[i - 1] = res[:, :, :, k * rows:(k + 1) * rows]
                send(qst.at[i - 1], qin.at[x], dev(xp(i), c, y), ("q", key))
            else:
                qin[x] = res[:, :, :, k * rows:(k + 1) * rows]
    up_send(1)
    for key in "LRO":
        arrived(rland.at[xof[key]], ("r1", key))
    rel = rland[0]
    for j in range(1, nx):
        rel = rel + rland[j]
    rfull[c] = rel
    send(rfull.at[c], rfull.at[c], sib, "r2")
    up_relay(0)
    arrived(rfull.at[1 - c], "r2")
    rel = rfull[...].reshape(n_slots, hw).astype(BF16).astype(F32)
    rel = jnp.broadcast_to(rel[:, None, :], (n_slots, n_heads, hw)).reshape(n_slots * n_heads, hw)
    col = lax.broadcasted_iota(jnp.int32, rel.shape, 1)
    row_head = lax.rem(lax.broadcasted_iota(jnp.int32, rel.shape, 0), n_heads)
    keep = (col >= row_head * hd) & (col < row_head * hd + hd)
    rel_diag[...] = jnp.where(keep, rel, 0.0).astype(BF16)
    c_k.wait()
    for key in "LRO":
        arrived(qin.at[xof[key]], ("q", key))
    outs = []
    for j in range(nx):
        outs.append(local(qin.at[j, :, 1], kn_ref.at[j * hx:(j + 1) * hx]))
        outs.append(local(qin.at[j, :, 2], vn_ref.at[j * hx:(j + 1) * hx]))
    pos = pos_ref[...]
    bu_t, bv_t = bu_ref[...].T, bv_ref[...].T
    scale = 1.0 / math.sqrt(hd)
    selfs, qvs = [], []
    for h in range(n_heads):
        q = qin[h // hx, h % hx, 0].astype(F32)
        qu = (q + bu_t[:, h:h + 1]).astype(BF16).astype(F32)
        qvs.append((q + bv_t[:, h:h + 1]).astype(BF16))
        selfs.append(jnp.sum(qu * qin[h // hx, h % hx, 1].astype(F32), axis=0, keepdims=True))
        for j in range(n_slots):
            s_ref[j, h:h + 1, :] = jnp.sum(kc[h, j].astype(F32) * qu, axis=0, keepdims=True)
    self_score = jnp.concatenate(selfs, axis=0)
    rel_all = dot(rel_diag[...], jnp.concatenate(qvs, axis=0), NN)
    rel_all = [rel_all[r * n_heads:(r + 1) * n_heads] for r in range(n_slots)][::-1]
    shift = n_slots - 1 - pos
    bit = 1
    while bit < n_slots:
        take = (shift // bit) % 2 == 1
        rel_all = [jnp.where(take, rel_all[j + bit], rel_all[j]) if j + bit < n_slots else rel_all[j] for j in range(n_slots)]
        bit *= 2
    sc = []
    for j in range(n_slots):
        content = jnp.where(pos == j, self_score, s_ref[j])
        sc.append(jnp.where(pos >= j, (content + rel_all[j]) * scale, -1e30))
    top = functools.reduce(jnp.maximum, sc)
    ex = [jnp.exp(v - top) for v in sc]
    tot = functools.reduce(jnp.add, ex)
    probs = [(v / tot).astype(BF16).astype(F32) for v in ex]
    self_prob = functools.reduce(jnp.add, [jnp.where(pos == j, probs[j], 0.0) for j in range(n_slots)])
    for j in range(n_slots):
        p_ref[j] = jnp.where(pos == j, 0.0, probs[j])
    p_ref[n_slots] = self_prob
    c_v.wait()
    for h in range(n_heads):
        acc = p_ref[n_slots, h:h + 1, :] * qin[h // hx, h % hx, 2].astype(F32)
        for j in range(n_slots):
            acc = acc + p_ref[j, h:h + 1, :] * vc[h, j].astype(F32)
        o_t[h * hd:(h + 1) * hd, :] = acc
    oall[x] = o_t[...].T.astype(BF16)
    half = rows // 2

    def o_unit(xx, h):
        return oall.at[xx, h * half:(h + 1) * half]

    x_start("o", o_unit)
    up_relay(1)
    c_wo.wait()
    arrived(wo_land.at[1 - c], "wo")
    wo[...] = jnp.concatenate([wo_land[0], wo_land[1]], axis=1)

    def out_proj(px):
        g = xof[px]
        part = dot(oall[g], wo[...], NN).astype(BF16)
        st1[g] = part.reshape(ny, qr, dx)
        for i, key in ((2, "O"), (1, "D"), (ny - 1, "U")):
            send(st1.at[g, yp(i)], in1.at[y, g], dev(x, c, yp(i)), ("r1y", px, key))
        in1[y, g] = st1[g, y]

    out_proj("S")
    x_relay("o", o_unit, "L")
    x_relay("o", o_unit, "R")
    up_send(2)
    x_wait("o", o_unit, "L", 1)
    out_proj("L")
    x_wait("o", o_unit, "R", 0)
    out_proj("R")
    x_wait("o", o_unit, "O", 0)
    x_wait("o", o_unit, "O", 1)
    out_proj("O")
    gain_m = jnp.concatenate([gall[2 * x, 1:2, :], gall[2 * x + 1, 1:2, :]], axis=1)
    for px in "SLRO":
        for key in "DUO":
            arrived(in1.at[yof[key], xof[px]], ("r1y", px, key))
    for g in range(nx):
        acc = in1[0, g].astype(F32)
        for k in range(1, ny):
            acc = acc + in1[k, g].astype(F32)
        acc = xall[g, rowsl(y * qr, qr), lanes(dx, x)].astype(F32) + acc
        for k in range(2):
            hbuf[k * half + g * hq:k * half + (g + 1) * hq, :] = acc[k * hq:(k + 1) * hq]
    h = hbuf[...]
    sq = jnp.sum(h * h, axis=1, keepdims=True)
    sq = jnp.broadcast_to(sq, (rows, rows)).T[:8]
    st_s[...] = sq
    st_r[x] = sq
    for i, key in ((2, "O"), (1, "L"), (nx - 1, "R")):
        send(st_s, st_r.at[x], dev(xp(i), c, y), ("st", key))
    up_send(3)
    for key in "LRO":
        arrived(st_r.at[xof[key]], ("st", key))
    tot = st_r[0]
    for j in range(1, nx):
        tot = tot + st_r[j]
    rstd = lax.rsqrt(tot * (1.0 / d_model) + NORM_EPS)
    rstd = jnp.broadcast_to(rstd[0:1], (rows, rows)).T[:, 0:1]
    mall[y, :, lanes(dx, x)] = (hbuf[...] * rstd * gain_m).astype(BF16)

    sub = half // 2

    def piece(h, k=None):
        return slice(h * half, (h + 1) * half) if k is None else slice(h * half + k * sub, h * half + (k + 1) * sub)

    def m_unit(px, py, h, k=None):
        return mall.at[yof[py], piece(h, k), lanes(dx, xof[px])]

    def z_unit(px, py, h, k=None):
        return zall.at[yof[py], piece(h, k), lanes(fx, xof[px])]

    def xs_send(name, unit, py, h):
        blk = unit("S", py, h)
        send(blk, blk, right, (name, py, h, "L"))
        send(blk, blk, left, (name, py, h, "R"))

    direct = set()

    def xs_direct(name, unit, py, h):
        direct.add((name, py, h))
        blk = unit("S", py, h)
        send(blk, blk, dev(xp(2), c, y), (name, py, h, "O"))
        xs_send(name, unit, py, h)

    def xs_near(name, unit, py, h):
        for frm in "LR":
            arrived(unit(frm, py, h), (name, py, h, frm))

    def xs_relay(name, unit, py, h):
        for frm, to, k in (("L", right, 0), ("R", left, 1)):
            arrived(unit(frm, py, h), (name, py, h, frm))
            blk = unit(frm, py, h, k)
            send(blk, blk, to, (name, py, h, "O", k))

    def xs_last(name, unit, py, h):
        if (name, py, h) in direct:
            arrived(unit("O", py, h), (name, py, h, "O"))
            return
        for k in range(2):
            arrived(unit("O", py, h, k), (name, py, h, "O", k))

    def ys_send(px, h):
        blk = m_unit(px, "S", h)
        send(blk, blk, above, ("my", px, h, "D"))
        send(blk, blk, below, ("my", px, h, "U"))

    def ys_relay(px, h):
        for frm, to, k in (("D", above, 0), ("U", below, 1)):
            arrived(m_unit(px, frm, h), ("my", px, h, frm))
            blk = m_unit(px, frm, h, k)
            send(blk, blk, to, ("my", px, h, "O", k))

    def ys_last(h):
        for px in "SLRO":
            for k in range(2):
                arrived(m_unit(px, "O", h, k), ("my", px, h, "O", k))

    def hidden(blocks, spread=xs_send):
        m = jnp.concatenate([mall[yof[py], piece(h), :] for py, h in blocks], axis=0)
        z = dot(m, wup[...].reshape(d_model, fx), NN)
        z = jax.nn.gelu(z, approximate=True).astype(BF16)
        for k, (py, h) in enumerate(blocks):
            zall[yof[py], piece(h), lanes(fx, x)] = z[k * half:(k + 1) * half]
            spread("z", z_unit, py, h)

    def down(blocks):
        for py, h in blocks:
            xs_last("z", z_unit, py, h)
        z = jnp.concatenate([zall[yof[py], piece(h), :] for py, h in blocks], axis=0)
        part = dot(z, wdn[...].reshape(dx, ff), NT).astype(BF16)
        for k, (py, h) in enumerate(blocks):
            blk = part[k * half:(k + 1) * half]
            if py == "S":
                in2[y, h] = blk
            else:
                j = "DUO".index(py)
                st2[j, h] = blk
                send(st2.at[j, h], in2.at[y, h], dev(x, c, yof[py]), ("r2y", {"D": "U", "U": "D", "O": "O"}[py], h))

    def y_unit(px, py, h):
        return yfull.at[yof[py], h * hq:(h + 1) * hq, lanes(dx, xof[px])]

    def yy_send(px, h):
        blk = y_unit(px, "S", h)
        for i, key in ((2, "O"), (1, "D"), (ny - 1, "U")):
            send(blk, blk, dev(x, c, yp(i)), ("yy", px, h, key))

    def finish(h):
        for key in "DUO":
            arrived(in2.at[yof[key], h], ("r2y", key, h))
        acc = in2[0, h].astype(F32)
        for k in range(1, ny):
            acc = acc + in2[k, h].astype(F32)
        yst[h] = (hbuf[piece(h), :] + acc).astype(BF16).reshape(nx, hq, dx)
        for i, key in ((2, "O"), (1, "L"), (nx - 1, "R")):
            send(yst.at[h, xp(i)], y_unit("S", "S", h), dev(xp(i), c, y), ("yx", key, h))
        yfull[y, h * hq:(h + 1) * hq, lanes(dx, x)] = yst[h, x]
        yy_send("S", h)

    def y_forward(h):
        for px in "LRO":
            arrived(y_unit(px, "S", h), ("yx", px, h))
            yy_send(px, h)

    xs_direct("mx", m_unit, "S", 0)
    ys_send("S", 0)
    xs_direct("mx", m_unit, "S", 1)
    ys_send("S", 1)
    up_relay(2)
    up_relay(3)
    xs_last("mx", m_unit, "S", 0)
    ys_send("O", 0)
    xs_near("mx", m_unit, "S", 0)
    ys_send("L", 0)
    ys_send("R", 0)
    c_up.wait()
    arrived(wup.at[2 * x + 1 - c], "uown")
    for p in range(4):
        for key in "LRO":
            arrived(wup.at[2 * xof[key] + 1 - c, UP_PARTS[p]:UP_PARTS[p + 1]], ("us", p, key))
    hidden([("S", 0)], xs_direct)
    xs_last("mx", m_unit, "S", 1)
    ys_send("O", 1)
    xs_near("mx", m_unit, "S", 1)
    ys_send("L", 1)
    ys_send("R", 1)
    hidden([("S", 1)], xs_direct)
    for px in "SOLR":
        ys_relay(px, 0)
    hidden([("D", 0), ("U", 0)])
    ys_last(0)
    hidden([("O", 0)])
    for px in "SLRO":
        ys_relay(px, 1)
    xs_relay("z", z_unit, "D", 0)
    xs_relay("z", z_unit, "U", 0)
    hidden([("D", 1), ("U", 1)])
    c_dn.wait()
    arrived(wdn.at[1 - c], "dn")
    xs_near("z", z_unit, "S", 0)
    xs_near("z", z_unit, "S", 1)
    down([("S", 0), ("S", 1)])
    xs_relay("z", z_unit, "O", 0)
    ys_last(1)
    hidden([("O", 1)])
    down([("D", 0), ("U", 0)])
    xs_relay("z", z_unit, "D", 1)
    xs_relay("z", z_unit, "U", 1)
    down([("O", 0)])
    xs_relay("z", z_unit, "O", 1)
    down([("D", 1), ("U", 1)])
    finish(0)
    down([("O", 1)])
    y_forward(0)
    finish(1)
    y_forward(1)
    for h in range(2):
        for px in "SLRO":
            for key in "DUO":
                arrived(y_unit(px, key, h), ("yy", px, h, key))
    outs.append(local(yfull, y_ref))
    for cp in pending:
        cp.wait_send()
    for cp in outs:
        cp.wait()
    assert len(ids) <= N_REMOTE and n_local[0] <= N_LOCAL


def copy_kernel(*refs):
    n = (len(refs) - 1) // 3
    srcs, dsts, bufs, sems = refs[:n], refs[n:2 * n], refs[2 * n:3 * n], refs[3 * n]
    ins = [pltpu.make_async_copy(srcs[i], bufs[i], sems.at[i]) for i in range(n)]
    outs = [pltpu.make_async_copy(bufs[i], dsts[i], sems.at[n + i]) for i in range(n)]
    for cp in ins:
        cp.start()
    for i in range(n):
        ins[i].wait()
        outs[i].start()
    for cp in outs:
        cp.wait()


def copy_out(*arrays):
    n = len(arrays)
    any_spec = pl.BlockSpec(memory_space=pl.ANY)
    return pl.pallas_call(
        copy_kernel,
        out_shape=tuple(jax.ShapeDtypeStruct(a.shape, a.dtype) for a in arrays),
        in_specs=[any_spec] * n,
        out_specs=tuple([any_spec] * n),
        scratch_shapes=[pltpu.VMEM(a.shape, a.dtype) for a in arrays] + [pltpu.SemaphoreType.DMA((2 * n,))],
    )(*arrays)


def solution(mesh):
    nx, ny = mesh.shape["wg"] // 2, mesh.shape["tp"]
    tok_axes = ("dp", "wg")
    in_specs = (P(tok_axes, None), P("wg"), P("wg"), P("wg", None, "tp", None), P("wg", "tp", None), P("tp", None, "wg"), P("wg", "tp"), P("tp", "wg"), P("tp", None), P("tp", None), P(None, None), P(tok_axes, "tp", None, None), P(tok_axes, "tp", None, None), P(tok_axes))
    out_specs = (P(tok_axes, None), P(tok_axes, "tp", None), P(tok_axes, "tp", None))

    def device_step(tokens, gain_attn, gain_mlp, w_qkv, w_rel, w_out, w_up, w_down, bias_u, bias_v, rel_table, k_cache, v_cache, positions):
        rows, d_model = tokens.shape
        ds = gain_attn.shape[0]
        dx = 2 * ds
        _, n_heads, n_slots, hd = k_cache.shape
        hx = n_heads // nx
        hw = n_heads * hd
        ff = w_up.shape[1]
        fx = ff // nx
        qr = rows // ny
        any_spec = pl.BlockSpec(memory_space=pl.ANY)
        vmem_spec = pl.BlockSpec(memory_space=pltpu.VMEM)
        vm = pltpu.VMEM
        scratch = [
            vm((nx, rows, d_model), BF16),
            vm((nx * rows, d_model), BF16),
            vm((2, 3 * hx * hd, 2 * rows), F32),
            vm((2, ds), F32),
            vm((2 * nx, 2, ds), F32),
            vm((1, d_model), F32),
            vm((2, 3, nx, hd, ds), BF16),
            vm((nx, 3 * hd, dx), BF16),
            vm((hx * 3 * hd, d_model), BF16),
            vm((nx - 1, hx, 3, hd, rows), BF16),
            vm((nx, hx, 3, hd, rows), BF16),
            vm((n_heads, n_slots, hd, rows), BF16),
            vm((n_heads, n_slots, hd, rows), BF16),
            vm((hw, ds), BF16),
            vm((2, n_slots // 2, hw), F32),
            vm((n_slots // 2, hw), F32),
            vm((nx, n_slots // 2, hw), F32),
            vm((2, n_slots // 2, hw), F32),
            vm((n_slots * n_heads, hw), BF16),
            vm((n_slots, n_heads, rows), F32),
            vm((n_slots + 1, n_heads, rows), F32),
            vm((hw, rows), F32),
            vm((nx, rows, hw), BF16),
            vm((2, hw, ds), BF16),
            vm((hw, dx), BF16),
            vm((nx, ny, qr, dx), BF16),
            vm((ny, nx, qr, dx), BF16),
            vm((rows, dx), F32),
            vm((8, rows), F32),
            vm((nx, 8, rows), F32),
            vm((ny, rows, d_model), BF16),
            vm((2 * nx, ds, fx), BF16),
            vm((ny, rows, ff), BF16),
            vm((2, ds, ff), BF16),
            vm((ny - 1, 2, rows // 2, dx), BF16),
            vm((ny, 2, rows // 2, dx), BF16),
            vm((2, nx, qr // 2, dx), BF16),
            vm((ny, qr, d_model), BF16),
            pltpu.SemaphoreType.DMA((N_REMOTE,)),
            pltpu.SemaphoreType.DMA((N_REMOTE,)),
            pltpu.SemaphoreType.DMA((N_LOCAL,)),
        ]
        y, kn, vn = pl.pallas_call(
            functools.partial(layer_kernel, nx, ny),
            out_shape=(
                jax.ShapeDtypeStruct((ny, qr, d_model), BF16),
                jax.ShapeDtypeStruct((n_heads, hd, rows), BF16),
                jax.ShapeDtypeStruct((n_heads, hd, rows), BF16),
            ),
            in_specs=[any_spec, vmem_spec, vmem_spec, any_spec, any_spec, any_spec, any_spec, any_spec, vmem_spec, vmem_spec, vmem_spec, any_spec, any_spec, vmem_spec],
            out_specs=(any_spec, any_spec, any_spec),
            scratch_shapes=scratch,
            compiler_params=pltpu.CompilerParams(collective_id=0, has_side_effects=True, vmem_limit_bytes=60 * 2**20),
        )(
            tokens, gain_attn, gain_mlp, w_qkv.transpose(1, 2, 3, 0).reshape(3, nx, hx, hd, ds), w_rel.transpose(1, 2, 0).reshape(hw, ds), w_out.reshape(hw, ds),
            w_up, w_down.T, bias_u, bias_v, rel_table, k_cache.transpose(1, 2, 3, 0), v_cache.transpose(1, 2, 3, 0), positions[None, :],
        )
        y, kn, vn = copy_out(y.reshape(rows, d_model), kn, vn)
        return y, kn.transpose(2, 0, 1), vn.transpose(2, 0, 1)

    return jax.shard_map(device_step, mesh=mesh, in_specs=in_specs, out_specs=out_specs, check_vma=False)
```

```python
import functools
import math

import jax
import jax.numpy as jnp
from jax import lax
from jax.experimental import pallas as pl
from jax.experimental.pallas import tpu as pltpu
from jax.sharding import PartitionSpec as P

MESH = pl.DeviceIdType.MESH
NORM_EPS = 1e-6
BF16 = jnp.bfloat16
F32 = jnp.float32
NT = (((1,), (1,)), ((), ()))
NN = (((1,), (0,)), ((), ()))
N_REMOTE = 256
N_LOCAL = 40
UP_PARTS = (0, 112, 160, 304, 320)


def dot(a, b, dims):
    return lax.dot_general(a, b, dims, preferred_element_type=F32)


def layer_kernel(nx, ny, tok_ref, ga_ref, gm_ref, wqkv_ref, wrel_ref, wout_ref, wup_ref, wdn_ref, bu_ref, bv_ref, relt_ref, kc_ref, vc_ref, pos_ref,
                 y_ref, kn_ref, vn_ref,
                 xall, nall, qacc, ga, gm, relt, bu, bv, posv, gall, gain, wq_land, wpk, wq, qst, qin, kc, vc, wrel, rsend, rsib, rland, rfull, rel_diag, s_ref, p_ref, o_t, oall, wo_land, wo,
                 st1, in1, hbuf, st_s, st_r, mall, wup, zall, wdn, st2, in2, yst, yfull,
                 ss, rs, ls):
    w = lax.axis_index("wg")
    x, c, y = w // 2, w % 2, lax.axis_index("tp")
    rows, d_model = tok_ref.shape
    ds = ga_ref.shape[0]
    dx = 2 * ds
    n_heads, n_slots, hd, _ = kc_ref.shape
    hx = n_heads // nx
    fx = wup_ref.shape[1] // nx
    qr = rows // ny
    hw = n_heads * hd
    ff = wup_ref.shape[1]

    def dev(xx, cc, yy):
        return {"wg": 2 * xx + cc, "tp": yy}

    def xp(i):
        return lax.rem(x + i, nx)

    def yp(i):
        return lax.rem(y + i, ny)

    sib = dev(x, 1 - c, y)
    right, left = dev(xp(1), c, y), dev(xp(nx - 1), c, y)
    above, below = dev(x, c, yp(1)), dev(x, c, yp(ny - 1))
    xof = {"S": x, "L": xp(nx - 1), "R": xp(1), "O": xp(2)}
    yof = {"S": y, "D": yp(ny - 1), "U": yp(1), "O": yp(2)}
    ids = {}
    pending = []
    n_local = [0]

    def nid(key):
        return ids.setdefault(key, len(ids))

    def send(src, dst, to, key):
        i = nid(key)
        cp = pltpu.make_async_remote_copy(src_ref=src, dst_ref=dst, send_sem=ss.at[i], recv_sem=rs.at[i], device_id=to, device_id_type=MESH)
        cp.start()
        pending.append(cp)

    def arrived(dst, key):
        i = nid(key)
        pltpu.make_async_remote_copy(src_ref=dst, dst_ref=dst, send_sem=ss.at[i], recv_sem=rs.at[i], device_id=sib, device_id_type=MESH).wait_recv()

    def local(src, dst):
        cp = pltpu.make_async_copy(src, dst, ls.at[n_local[0]])
        n_local[0] += 1
        cp.start()
        return cp

    def lanes(size, k):
        return pl.ds(pl.multiple_of(k * size, 128), size)

    def rowsl(start, size):
        return pl.ds(pl.multiple_of(start, 16), size)

    def x_start(name, unit):
        for h, to, frm in ((0, right, "L"), (1, left, "R"), (1, right, "L"), (0, left, "R")):
            send(unit(x, h), unit(x, h), to, (name, frm, h))

    def x_relay(name, unit, frm):
        h, to = (0, right) if frm == "L" else (1, left)
        arrived(unit(xof[frm], h), (name, frm, h))
        send(unit(xof[frm], h), unit(xof[frm], h), to, (name, "O", h))

    def x_wait(name, unit, frm, h):
        arrived(unit(xof[frm], h), (name, frm, h))

    def y_send(name, unit, px, h):
        blk = unit(xof[px], y, h)
        send(blk, blk, above, (name, px, "D", h))
        send(blk, blk, below, (name, px, "U", h))

    def y_relay(name, unit, px, frm):
        h, to = (0, above) if frm == "D" else (1, below)
        blk = unit(xof[px], yof[frm], h)
        arrived(blk, (name, px, frm, h))
        send(blk, blk, to, (name, px, "O", h))

    def y_wait(name, unit, px, frm, h):
        arrived(unit(xof[px], yof[frm], h), (name, px, frm, h))

    barrier = pltpu.get_barrier_semaphore()
    peers = [dev(xp(i), c, y) for i in range(1, nx)] + [dev(x, c, yp(i)) for i in range(1, ny)] + [sib]
    for peer in peers:
        pl.semaphore_signal(barrier, inc=1, device_id=peer, device_id_type=MESH)
    c_small = [local(ga_ref, ga), local(gm_ref, gm)]
    c_rel = [local(wrel_ref, wrel), local(relt_ref.at[:, lanes(dx, x)], relt)]
    c_x = local(tok_ref, xall.at[x])
    c_wq = local(wqkv_ref.at[:, :, c], wq_land.at[c])
    c_bias = [local(bu_ref, bu), local(bv_ref, bv), local(pos_ref, posv)]
    c_k = local(kc_ref, kc)
    c_v = local(vc_ref, vc)
    c_wo = local(wout_ref, wo_land.at[c])
    c_up = local(wup_ref.at[:, lanes(fx, x)], wup.at[w])
    c_dn = local(wdn_ref, wdn.at[c])
    for cp in c_rel:
        cp.wait()
    tab = jnp.where(c == 0, relt[:, :ds], relt[:, ds:])
    hs = n_slots // 2
    rsend[...] = dot(tab, wrel[...], NT).reshape(2, hs, hw)
    for cp in c_small:
        cp.wait()
    gall[w, 0:1, :] = ga[...].reshape(1, ds)
    gall[w, 1:2, :] = gm[...].reshape(1, ds)

    pl.semaphore_wait(barrier, len(peers))

    hq = qr // 2

    def tok_unit(xx, yy, h):
        return xall.at[xx, rowsl(yy * qr + h * hq, hq)]

    def tok_x(xx, h):
        return tok_unit(xx, y, h)

    c_x.wait()
    x_start("tx", tok_x)
    send(wqkv_ref.at[:, :, 1 - c], wq_land.at[c], sib, "wqs")
    send(gall.at[w], gall.at[w], sib, ("g", 0))
    for i in range(1, nx):
        send(gall.at[w], gall.at[w], dev(xp(i), c, y), ("g", i))
    send(rsend.at[1 - c], rsib, sib, "r0")
    x_relay("tx", tok_x, "L")
    y_send("ty", tok_unit, "L", 0)
    x_relay("tx", tok_x, "R")
    y_send("ty", tok_unit, "R", 1)
    c_wq.wait()
    arrived(wq_land.at[1 - c], "wqs")
    for s in range(3):
        for j in range(nx):
            wpk[j, s * hd:(s + 1) * hd, :] = jnp.concatenate([wq_land[0, s, j], wq_land[1, s, j]], axis=1)

    def wq_unit(cc, xx):
        return wq.at[rowsl(cc * (3 * hd), 3 * hd), lanes(dx, xx)]

    for i, key in ((1, "L"), (nx - 1, "R"), (2, "O")):
        send(wpk.at[xp(i)], wq_unit(c, x), dev(xp(i), c, y), ("wx", key))
    wq[rowsl(c * (3 * hd), 3 * hd), lanes(dx, x)] = wpk[x]
    send(wpk.at[x], wq_unit(c, x), sib, ("ws", "S"))
    arrived(rsib, "r0")
    rland[x] = rsend[c] + rsib[...]
    for i, key in ((1, "L"), (nx - 1, "R"), (2, "O")):
        send(rland.at[x], rland.at[x], dev(xp(i), c, y), ("r1", key))
    for frm, h in (("L", 1), ("R", 0), ("O", 0), ("O", 1)):
        x_wait("tx", tok_x, frm, h)
        y_send("ty", tok_unit, frm, h)

    def up_send(p):
        r0, r1 = UP_PARTS[p], UP_PARTS[p + 1]
        for i, key in ((1, "L"), (nx - 1, "R"), (2, "O")):
            send(wup_ref.at[r0:r1, lanes(fx, xp(i))], wup.at[w, r0:r1], dev(xp(i), c, y), ("ux", p, key))

    def up_relay(p):
        r0, r1 = UP_PARTS[p], UP_PARTS[p + 1]
        for key in "LRO":
            blk = wup.at[2 * xof[key] + c, r0:r1]
            arrived(blk, ("ux", p, key))
            send(blk, blk, sib, ("us", p, key))

    up_send(0)
    send(wout_ref, wo_land.at[c], sib, "wo")
    send(wdn_ref, wdn.at[c], sib, "dn")
    send(wup_ref.at[:, lanes(fx, x)], wup.at[w], sib, "uown")
    for i in range(1, nx):
        blk = gall.at[2 * lax.rem(x + nx - i, nx) + c]
        arrived(blk, ("g", i))
        send(blk, blk, sib, ("gs", i))
    arrived(gall.at[2 * x + 1 - c], ("g", 0))
    for i in range(1, nx):
        arrived(gall.at[2 * lax.rem(x + nx - i, nx) + 1 - c], ("gs", i))
    gain[...] = jnp.concatenate([gall[j, 0:1, :] for j in range(2 * nx)], axis=1)
    def norm_block(px, yy):
        v = xall[xof[px], rowsl(yy * qr, qr), :].astype(F32)
        ms = jnp.mean(v * v, axis=-1, keepdims=True)
        nall[rowsl("ORLS".index(px) * rows + yy * qr, qr), :] = (v * lax.rsqrt(ms + NORM_EPS) * gain[...]).astype(BF16)

    def norm_own(r, carry):
        norm_block("S", r)
        return carry

    lax.fori_loop(0, ny, norm_own, 0)
    for px in "LRO":
        norm_block(px, y)
    for px, frm in (("L", "D"), ("R", "U"), ("L", "U"), ("R", "D"), ("O", "D"), ("O", "U")):
        y_relay("ty", tok_unit, px, frm)
    for px in "LRO":
        y_wait("ty", tok_unit, px, "D", 1)
        norm_block(px, yof["D"])
        y_wait("ty", tok_unit, px, "U", 0)
        norm_block(px, yof["U"])
    def qkv_part(key, p):
        k = lanes(dx, xof[key])
        return dot(wq[:, k], nall[2 * p * rows:2 * (p + 1) * rows, k], NT)

    def wq_relay(key):
        arrived(wq_unit(c, xof[key]), ("wx", key))
        send(wq_unit(c, xof[key]), wq_unit(c, xof[key]), sib, ("ws", key))

    wq_relay("L")
    wq_relay("R")
    wq_relay("O")
    for px in "LRO":
        y_wait("ty", tok_unit, px, "O", 0)
        y_wait("ty", tok_unit, px, "O", 1)
        norm_block(px, yof["O"])
    arrived(wq_unit(1 - c, x), ("ws", "S"))
    for p in range(2):
        qacc[p] = qkv_part("S", p)
    for key in "LR":
        arrived(wq_unit(1 - c, xof[key]), ("ws", key))
    for p in range(2):
        qacc[p] += qkv_part("L", p) + qkv_part("R", p)
    arrived(wq_unit(1 - c, xof["O"]), ("ws", "O"))
    for p, pair in enumerate((((2, "O"), (1, "L")), ((nx - 1, "R"), (0, "S")))):
        res = (qacc[p] + qkv_part("O", p)).astype(BF16).reshape(hx, 3, hd, 2 * rows)
        for k, (i, key) in enumerate(pair):
            if i:
                qst[i - 1] = res[:, :, :, k * rows:(k + 1) * rows]
                send(qst.at[i - 1, :, 0:2], qin.at[x, :, 0:2], dev(xp(i), c, y), ("q", key))
            else:
                qin[x] = res[:, :, :, k * rows:(k + 1) * rows]
    for i, key in ((2, "O"), (1, "L"), (nx - 1, "R")):
        send(qst.at[i - 1, :, 2], qin.at[x, :, 2], dev(xp(i), c, y), ("v", key))
    up_send(1)
    for key in "LRO":
        arrived(rland.at[xof[key]], ("r1", key))
    rel = rland[0]
    for j in range(1, nx):
        rel = rel + rland[j]
    rfull[c] = rel
    send(rfull.at[c], rfull.at[c], sib, "r2")
    up_relay(0)
    arrived(rfull.at[1 - c], "r2")
    rel = rfull[...].reshape(n_slots, hw).astype(BF16).astype(F32)
    rel = jnp.broadcast_to(rel[:, None, :], (n_slots, n_heads, hw)).reshape(n_slots * n_heads, hw)
    col = lax.broadcasted_iota(jnp.int32, rel.shape, 1)
    row_head = lax.rem(lax.broadcasted_iota(jnp.int32, rel.shape, 0), n_heads)
    keep = (col >= row_head * hd) & (col < row_head * hd + hd)
    rel_diag[...] = jnp.where(keep, rel, 0.0).astype(BF16)
    c_k.wait()
    for key in "LRO":
        arrived(qin.at[xof[key], :, 0:2], ("q", key))
    outs = []
    for j in range(nx):
        outs.append(local(qin.at[j, :, 1], kn_ref.at[j * hx:(j + 1) * hx]))
    for cp in c_bias:
        cp.wait()
    pos = posv[...]
    bu_t, bv_t = bu[...].T, bv[...].T
    scale = 1.0 / math.sqrt(hd)
    selfs, qvs = [], []
    for h in range(n_heads):
        q = qin[h // hx, h % hx, 0].astype(F32)
        qu = (q + bu_t[:, h:h + 1]).astype(BF16).astype(F32)
        qvs.append((q + bv_t[:, h:h + 1]).astype(BF16))
        selfs.append(jnp.sum(qu * qin[h // hx, h % hx, 1].astype(F32), axis=0, keepdims=True))
        for j in range(n_slots):
            s_ref[j, h:h + 1, :] = jnp.sum(kc[h, j].astype(F32) * qu, axis=0, keepdims=True)
    self_score = jnp.concatenate(selfs, axis=0)
    rel_all = dot(rel_diag[...], jnp.concatenate(qvs, axis=0), NN)
    rel_all = [rel_all[r * n_heads:(r + 1) * n_heads] for r in range(n_slots)][::-1]
    shift = n_slots - 1 - pos
    bit = 1
    while bit < n_slots:
        take = (shift // bit) % 2 == 1
        rel_all = [jnp.where(take, rel_all[j + bit], rel_all[j]) if j + bit < n_slots else rel_all[j] for j in range(n_slots)]
        bit *= 2
    sc = []
    for j in range(n_slots):
        content = jnp.where(pos == j, self_score, s_ref[j])
        sc.append(jnp.where(pos >= j, (content + rel_all[j]) * scale, -1e30))
    top = functools.reduce(jnp.maximum, sc)
    ex = [jnp.exp(v - top) for v in sc]
    tot = functools.reduce(jnp.add, ex)
    probs = [(v / tot).astype(BF16).astype(F32) for v in ex]
    self_prob = functools.reduce(jnp.add, [jnp.where(pos == j, probs[j], 0.0) for j in range(n_slots)])
    for j in range(n_slots):
        p_ref[j] = jnp.where(pos == j, 0.0, probs[j])
    p_ref[n_slots] = self_prob
    c_v.wait()
    for key in "LRO":
        arrived(qin.at[xof[key], :, 2], ("v", key))
    for j in range(nx):
        outs.append(local(qin.at[j, :, 2], vn_ref.at[j * hx:(j + 1) * hx]))
    for h in range(n_heads):
        acc = p_ref[n_slots, h:h + 1, :] * qin[h // hx, h % hx, 2].astype(F32)
        for j in range(n_slots):
            acc = acc + p_ref[j, h:h + 1, :] * vc[h, j].astype(F32)
        o_t[h * hd:(h + 1) * hd, :] = acc
    oall[x] = o_t[...].T.astype(BF16)
    half = rows // 2

    oq = rows // 4

    def o_unit(px, k0, n):
        return oall.at[xof[px], k0 * oq:(k0 + n) * oq]

    for k0, n, to, frm in ((0, 1, right, "L"), (2, 1, left, "R"), (1, 1, right, "L"), (3, 1, left, "R"), (2, 2, right, "L"), (0, 2, left, "R")):
        send(o_unit("S", k0, n), o_unit("S", k0, n), to, ("o", frm, k0))
    c_wo.wait()
    arrived(wo_land.at[1 - c], "wo")
    wo[...] = jnp.concatenate([wo_land[0], wo_land[1]], axis=1)

    def out_proj(px):
        g = xof[px]
        part = dot(oall[g], wo[...], NN).astype(BF16)
        st1[g] = part.reshape(ny, qr, dx)
        for i, key in ((2, "O"), (1, "D"), (ny - 1, "U")):
            send(st1.at[g, yp(i)], in1.at[y, g], dev(x, c, yp(i)), ("r1y", px, key))
        in1[y, g] = st1[g, y]

    out_proj("S")
    for frm, k, to in (("L", 0, right), ("R", 2, left), ("L", 1, right), ("R", 3, left)):
        arrived(o_unit(frm, k, 1), ("o", frm, k))
        send(o_unit(frm, k, 1), o_unit(frm, k, 1), to, ("o", "O", k))
    up_send(2)
    arrived(o_unit("L", 2, 2), ("o", "L", 2))
    out_proj("L")
    arrived(o_unit("R", 0, 2), ("o", "R", 0))
    out_proj("R")
    for k in range(4):
        arrived(o_unit("O", k, 1), ("o", "O", k))
    out_proj("O")
    up_relay(1)
    gain_m = jnp.concatenate([gall[2 * x, 1:2, :], gall[2 * x + 1, 1:2, :]], axis=1)
    for px in "SLRO":
        for key in "DUO":
            arrived(in1.at[yof[key], xof[px]], ("r1y", px, key))
    for g in range(nx):
        acc = in1[0, g].astype(F32)
        for k in range(1, ny):
            acc = acc + in1[k, g].astype(F32)
        acc = xall[g, rowsl(y * qr, qr), lanes(dx, x)].astype(F32) + acc
        for k in range(2):
            hbuf[k * half + g * hq:k * half + (g + 1) * hq, :] = acc[k * hq:(k + 1) * hq]
    h = hbuf[...]
    sq = jnp.sum(h * h, axis=1, keepdims=True)
    sq = jnp.broadcast_to(sq, (rows, rows)).T[:8]
    st_s[...] = sq
    st_r[x] = sq
    for i, key in ((2, "O"), (1, "L"), (nx - 1, "R")):
        send(st_s, st_r.at[x], dev(xp(i), c, y), ("st", key))
    up_send(3)
    for key in "LRO":
        arrived(st_r.at[xof[key]], ("st", key))
    tot = st_r[0]
    for j in range(1, nx):
        tot = tot + st_r[j]
    rstd = lax.rsqrt(tot * (1.0 / d_model) + NORM_EPS)
    rstd = jnp.broadcast_to(rstd[0:1], (rows, rows)).T[:, 0:1]
    mall[y, :, lanes(dx, x)] = (hbuf[...] * rstd * gain_m).astype(BF16)

    sub = half // 2

    def piece(h, k=None):
        return slice(h * half, (h + 1) * half) if k is None else slice(h * half + k * sub, h * half + (k + 1) * sub)

    def m_unit(px, py, h, k=None):
        return mall.at[yof[py], piece(h, k), lanes(dx, xof[px])]

    def z_unit(px, py, h, k=None):
        return zall.at[yof[py], piece(h, k), lanes(fx, xof[px])]

    def xs_send(name, unit, py, h):
        blk = unit("S", py, h)
        send(blk, blk, right, (name, py, h, "L"))
        send(blk, blk, left, (name, py, h, "R"))

    direct = set()

    def xs_direct(name, unit, py, h):
        direct.add((name, py, h))
        blk = unit("S", py, h)
        send(blk, blk, dev(xp(2), c, y), (name, py, h, "O"))
        xs_send(name, unit, py, h)

    def xs_near(name, unit, py, h):
        for frm in "LR":
            arrived(unit(frm, py, h), (name, py, h, frm))

    def xs_relay(name, unit, py, h):
        for frm, to, k in (("L", right, 0), ("R", left, 1)):
            arrived(unit(frm, py, h), (name, py, h, frm))
            blk = unit(frm, py, h, k)
            send(blk, blk, to, (name, py, h, "O", k))

    def xs_last(name, unit, py, h):
        if (name, py, h) in direct:
            arrived(unit("O", py, h), (name, py, h, "O"))
            return
        for k in range(2):
            arrived(unit("O", py, h, k), (name, py, h, "O", k))

    def ys_send(px, h):
        blk = m_unit(px, "S", h)
        send(blk, blk, above, ("my", px, h, "D"))
        send(blk, blk, below, ("my", px, h, "U"))

    def ys_relay(px, h):
        for frm, to, k in (("D", above, 0), ("U", below, 1)):
            arrived(m_unit(px, frm, h), ("my", px, h, frm))
            blk = m_unit(px, frm, h, k)
            send(blk, blk, to, ("my", px, h, "O", k))

    def ys_last(h):
        for px in "SLRO":
            for k in range(2):
                arrived(m_unit(px, "O", h, k), ("my", px, h, "O", k))

    def hidden(blocks, spread=xs_send):
        m = jnp.concatenate([mall[yof[py], piece(h), :] for py, h in blocks], axis=0)
        z = dot(m, wup[...].reshape(d_model, fx), NN)
        z = jax.nn.gelu(z, approximate=True).astype(BF16)
        for k, (py, h) in enumerate(blocks):
            zall[yof[py], piece(h), lanes(fx, x)] = z[k * half:(k + 1) * half]
            spread("z", z_unit, py, h)

    def down(blocks):
        for py, h in blocks:
            xs_last("z", z_unit, py, h)
        z = jnp.concatenate([zall[yof[py], piece(h), :] for py, h in blocks], axis=0)
        part = dot(z, wdn[...].reshape(dx, ff), NT).astype(BF16)
        for k, (py, h) in enumerate(blocks):
            blk = part[k * half:(k + 1) * half]
            if py == "S":
                in2[y, h] = blk
            else:
                j = "DUO".index(py)
                st2[j, h] = blk
                send(st2.at[j, h], in2.at[y, h], dev(x, c, yof[py]), ("r2y", {"D": "U", "U": "D", "O": "O"}[py], h))

    def y_unit(px, h):
        return yfull.at[h * hq:(h + 1) * hq, lanes(dx, xof[px])]

    def y_out(px, py, h):
        return y_ref.at[yof[py], h * hq:(h + 1) * hq, lanes(dx, xof[px])]

    def yy_send(px, h):
        for i, key in ((2, "O"), (1, "D"), (ny - 1, "U")):
            send(y_unit(px, h), y_out(px, "S", h), dev(x, c, yp(i)), ("yy", px, h, key))
        outs.append(local(y_unit(px, h), y_out(px, "S", h)))

    def finish(h):
        for key in "DUO":
            arrived(in2.at[yof[key], h], ("r2y", key, h))
        acc = in2[0, h].astype(F32)
        for k in range(1, ny):
            acc = acc + in2[k, h].astype(F32)
        yst[h] = (hbuf[piece(h), :] + acc).astype(BF16).reshape(nx, hq, dx)
        for i, key in ((2, "O"), (1, "L"), (nx - 1, "R")):
            send(yst.at[h, xp(i)], y_unit("S", h), dev(xp(i), c, y), ("yx", key, h))
        yfull[h * hq:(h + 1) * hq, lanes(dx, x)] = yst[h, x]
        yy_send("S", h)

    def y_forward(h):
        for px in "LRO":
            arrived(y_unit(px, h), ("yx", px, h))
            yy_send(px, h)

    xs_direct("mx", m_unit, "S", 0)
    ys_send("S", 0)
    xs_direct("mx", m_unit, "S", 1)
    ys_send("S", 1)
    up_relay(2)
    up_relay(3)
    xs_last("mx", m_unit, "S", 0)
    ys_send("O", 0)
    xs_near("mx", m_unit, "S", 0)
    ys_send("L", 0)
    ys_send("R", 0)
    c_up.wait()
    arrived(wup.at[2 * x + 1 - c], "uown")
    for p in range(4):
        for key in "LRO":
            arrived(wup.at[2 * xof[key] + 1 - c, UP_PARTS[p]:UP_PARTS[p + 1]], ("us", p, key))
    hidden([("S", 0)], xs_direct)
    xs_last("mx", m_unit, "S", 1)
    xs_near("mx", m_unit, "S", 1)
    hidden([("S", 1)])
    for px in "SOLR":
        ys_relay(px, 0)
    for px in "OLR":
        ys_send(px, 1)
    hidden([("D", 0), ("U", 0)])
    xs_relay("z", z_unit, "S", 1)
    ys_last(0)
    hidden([("O", 0)])
    for px in "SLRO":
        ys_relay(px, 1)
    xs_relay("z", z_unit, "D", 0)
    xs_relay("z", z_unit, "U", 0)
    hidden([("D", 1), ("U", 1)])
    c_dn.wait()
    arrived(wdn.at[1 - c], "dn")
    xs_near("z", z_unit, "S", 0)
    down([("S", 0), ("S", 1)])
    xs_relay("z", z_unit, "O", 0)
    ys_last(1)
    hidden([("O", 1)])
    down([("D", 0), ("U", 0)])
    xs_relay("z", z_unit, "D", 1)
    xs_relay("z", z_unit, "U", 1)
    down([("O", 0)])
    xs_relay("z", z_unit, "O", 1)
    down([("D", 1), ("U", 1)])
    down([("O", 1)])
    finish(0)
    y_forward(0)
    finish(1)
    y_forward(1)
    for h in range(2):
        for px in "SLRO":
            for key in "DUO":
                arrived(y_out(px, key, h), ("yy", px, h, key))
    for cp in pending:
        cp.wait_send()
    for cp in outs:
        cp.wait()
    assert len(ids) <= N_REMOTE and n_local[0] <= N_LOCAL


def copy_kernel(*refs):
    n = (len(refs) - 1) // 3
    srcs, dsts, bufs, sems = refs[:n], refs[n:2 * n], refs[2 * n:3 * n], refs[3 * n]
    ins = [pltpu.make_async_copy(srcs[i], bufs[i], sems.at[i]) for i in range(n)]
    outs = [pltpu.make_async_copy(bufs[i], dsts[i], sems.at[n + i]) for i in range(n)]
    for cp in ins:
        cp.start()
    for i in range(n):
        ins[i].wait()
        outs[i].start()
    for cp in outs:
        cp.wait()


def copy_out(*arrays):
    n = len(arrays)
    any_spec = pl.BlockSpec(memory_space=pl.ANY)
    return pl.pallas_call(
        copy_kernel,
        out_shape=tuple(jax.ShapeDtypeStruct(a.shape, a.dtype) for a in arrays),
        in_specs=[any_spec] * n,
        out_specs=tuple([any_spec] * n),
        scratch_shapes=[pltpu.VMEM(a.shape, a.dtype) for a in arrays] + [pltpu.SemaphoreType.DMA((2 * n,))],
    )(*arrays)


def solution(mesh):
    nx, ny = mesh.shape["wg"] // 2, mesh.shape["tp"]
    tok_axes = ("dp", "wg")
    in_specs = (P(tok_axes, None), P("wg"), P("wg"), P("wg", None, "tp", None), P("wg", "tp", None), P("tp", None, "wg"), P("wg", "tp"), P("tp", "wg"), P("tp", None), P("tp", None), P(None, None), P(tok_axes, "tp", None, None), P(tok_axes, "tp", None, None), P(tok_axes))
    out_specs = (P(tok_axes, None), P(tok_axes, "tp", None), P(tok_axes, "tp", None))

    def device_step(tokens, gain_attn, gain_mlp, w_qkv, w_rel, w_out, w_up, w_down, bias_u, bias_v, rel_table, k_cache, v_cache, positions):
        rows, d_model = tokens.shape
        ds = gain_attn.shape[0]
        dx = 2 * ds
        _, n_heads, n_slots, hd = k_cache.shape
        hx = n_heads // nx
        hw = n_heads * hd
        ff = w_up.shape[1]
        fx = ff // nx
        qr = rows // ny
        any_spec = pl.BlockSpec(memory_space=pl.ANY)
        vm = pltpu.VMEM
        scratch = [
            vm((nx, rows, d_model), BF16),
            vm((nx * rows, d_model), BF16),
            vm((2, 3 * hx * hd, 2 * rows), F32),
            vm((ds,), F32),
            vm((ds,), F32),
            vm((n_slots, dx), BF16),
            vm((n_heads, hd), F32),
            vm((n_heads, hd), F32),
            vm((1, rows), jnp.int32),
            vm((2 * nx, 2, ds), F32),
            vm((1, d_model), F32),
            vm((2, 3, nx, hd, ds), BF16),
            vm((nx, 3 * hd, dx), BF16),
            vm((hx * 3 * hd, d_model), BF16),
            vm((nx - 1, hx, 3, hd, rows), BF16),
            vm((nx, hx, 3, hd, rows), BF16),
            vm((n_heads, n_slots, hd, rows), BF16),
            vm((n_heads, n_slots, hd, rows), BF16),
            vm((hw, ds), BF16),
            vm((2, n_slots // 2, hw), F32),
            vm((n_slots // 2, hw), F32),
            vm((nx, n_slots // 2, hw), F32),
            vm((2, n_slots // 2, hw), F32),
            vm((n_slots * n_heads, hw), BF16),
            vm((n_slots, n_heads, rows), F32),
            vm((n_slots + 1, n_heads, rows), F32),
            vm((hw, rows), F32),
            vm((nx, rows, hw), BF16),
            vm((2, hw, ds), BF16),
            vm((hw, dx), BF16),
            vm((nx, ny, qr, dx), BF16),
            vm((ny, nx, qr, dx), BF16),
            vm((rows, dx), F32),
            vm((8, rows), F32),
            vm((nx, 8, rows), F32),
            vm((ny, rows, d_model), BF16),
            vm((2 * nx, ds, fx), BF16),
            vm((ny, rows, ff), BF16),
            vm((2, ds, ff), BF16),
            vm((ny - 1, 2, rows // 2, dx), BF16),
            vm((ny, 2, rows // 2, dx), BF16),
            vm((2, nx, qr // 2, dx), BF16),
            vm((qr, d_model), BF16),
            pltpu.SemaphoreType.DMA((N_REMOTE,)),
            pltpu.SemaphoreType.DMA((N_REMOTE,)),
            pltpu.SemaphoreType.DMA((N_LOCAL,)),
        ]
        y, kn, vn = pl.pallas_call(
            functools.partial(layer_kernel, nx, ny),
            out_shape=(
                jax.ShapeDtypeStruct((ny, qr, d_model), BF16),
                jax.ShapeDtypeStruct((n_heads, hd, rows), BF16),
                jax.ShapeDtypeStruct((n_heads, hd, rows), BF16),
            ),
            in_specs=[any_spec] * 14,
            out_specs=(any_spec, any_spec, any_spec),
            scratch_shapes=scratch,
            compiler_params=pltpu.CompilerParams(collective_id=0, has_side_effects=True, vmem_limit_bytes=60 * 2**20),
        )(
            tokens, gain_attn, gain_mlp, w_qkv.transpose(1, 2, 3, 0).reshape(3, nx, hx, hd, ds), w_rel.transpose(1, 2, 0).reshape(hw, ds), w_out.reshape(hw, ds),
            w_up, w_down.T, bias_u, bias_v, rel_table, k_cache.transpose(1, 2, 3, 0), v_cache.transpose(1, 2, 3, 0), positions[None, :],
        )
        y, kn, vn = copy_out(y.reshape(rows, d_model), kn, vn)
        return y, kn.transpose(2, 0, 1), vn.transpose(2, 0, 1)

    return jax.shard_map(device_step, mesh=mesh, in_specs=in_specs, out_specs=out_specs, check_vma=False)
```

```python
import functools
import math

import jax
import jax.numpy as jnp
from jax import lax
from jax.experimental import pallas as pl
from jax.experimental.pallas import tpu as pltpu
from jax.sharding import PartitionSpec as P

MESH = pl.DeviceIdType.MESH
NORM_EPS = 1e-6
BF16 = jnp.bfloat16
F32 = jnp.float32
NT = (((1,), (1,)), ((), ()))
NN = (((1,), (0,)), ((), ()))
N_REMOTE = 256
N_LOCAL = 40
UP_PARTS = (0, 112, 160, 304, 320)


def dot(a, b, dims):
    return lax.dot_general(a, b, dims, preferred_element_type=F32)


def layer_kernel(nx, ny, tok_ref, ga_ref, gm_ref, wqkv_ref, wrel_ref, wout_ref, wup_ref, wdn_ref, bu_ref, bv_ref, relt_ref, kc_ref, vc_ref, pos_ref,
                 y_ref, kn_ref, vn_ref,
                 xall, nall, qacc, ga, gm, relt, bu, bv, posv, gall, gain, wq_land, wpk, wq, qst, qin, kc, vc, wrel, rsend, rsib, rland, rfull, rel_diag, s_ref, p_ref, o_t, oall, wo_land, wo,
                 st1, in1, hbuf, st_s, st_r, mall, wup, zall, wdn, st2, in2, yst, yfull,
                 ss, rs, ls):
    w = lax.axis_index("wg")
    x, c, y = w // 2, w % 2, lax.axis_index("tp")
    rows, d_model = tok_ref.shape
    ds = ga_ref.shape[0]
    dx = 2 * ds
    n_heads, n_slots, hd, _ = kc_ref.shape
    hx = n_heads // nx
    fx = wup_ref.shape[1] // nx
    qr = rows // ny
    hw = n_heads * hd
    ff = wup_ref.shape[1]

    def dev(xx, cc, yy):
        return {"wg": 2 * xx + cc, "tp": yy}

    def xp(i):
        return lax.rem(x + i, nx)

    def yp(i):
        return lax.rem(y + i, ny)

    sib = dev(x, 1 - c, y)
    right, left = dev(xp(1), c, y), dev(xp(nx - 1), c, y)
    above, below = dev(x, c, yp(1)), dev(x, c, yp(ny - 1))
    xof = {"S": x, "L": xp(nx - 1), "R": xp(1), "O": xp(2)}
    yof = {"S": y, "D": yp(ny - 1), "U": yp(1), "O": yp(2)}
    ids = {}
    pending = []
    n_local = [0]

    def nid(key):
        return ids.setdefault(key, len(ids))

    def send(src, dst, to, key):
        i = nid(key)
        cp = pltpu.make_async_remote_copy(src_ref=src, dst_ref=dst, send_sem=ss.at[i], recv_sem=rs.at[i], device_id=to, device_id_type=MESH)
        cp.start()
        pending.append(cp)

    def arrived(dst, key):
        i = nid(key)
        pltpu.make_async_remote_copy(src_ref=dst, dst_ref=dst, send_sem=ss.at[i], recv_sem=rs.at[i], device_id=sib, device_id_type=MESH).wait_recv()

    def local(src, dst):
        cp = pltpu.make_async_copy(src, dst, ls.at[n_local[0]])
        n_local[0] += 1
        cp.start()
        return cp

    def lanes(size, k):
        return pl.ds(pl.multiple_of(k * size, 128), size)

    def rowsl(start, size):
        return pl.ds(pl.multiple_of(start, 16), size)

    def x_start(name, unit):
        for h, to, frm in ((0, right, "L"), (1, left, "R"), (1, right, "L"), (0, left, "R")):
            send(unit(x, h), unit(x, h), to, (name, frm, h))

    def x_relay(name, unit, frm):
        h, to = (0, right) if frm == "L" else (1, left)
        arrived(unit(xof[frm], h), (name, frm, h))
        send(unit(xof[frm], h), unit(xof[frm], h), to, (name, "O", h))

    def x_wait(name, unit, frm, h):
        arrived(unit(xof[frm], h), (name, frm, h))

    def y_send(name, unit, px, h):
        blk = unit(xof[px], y, h)
        send(blk, blk, above, (name, px, "D", h))
        send(blk, blk, below, (name, px, "U", h))

    def y_relay(name, unit, px, frm):
        h, to = (0, above) if frm == "D" else (1, below)
        blk = unit(xof[px], yof[frm], h)
        arrived(blk, (name, px, frm, h))
        send(blk, blk, to, (name, px, "O", h))

    def y_wait(name, unit, px, frm, h):
        arrived(unit(xof[px], yof[frm], h), (name, px, frm, h))

    barrier = pltpu.get_barrier_semaphore()
    peers = [dev(xp(i), c, y) for i in range(1, nx)] + [dev(x, c, yp(i)) for i in range(1, ny)] + [sib]
    for peer in peers:
        pl.semaphore_signal(barrier, inc=1, device_id=peer, device_id_type=MESH)
    c_small = [local(ga_ref, ga), local(gm_ref, gm)]
    c_rel = [local(wrel_ref, wrel), local(relt_ref.at[:, lanes(dx, x)], relt)]
    c_x = local(tok_ref, xall.at[x])
    c_wq = local(wqkv_ref.at[:, :, c], wq_land.at[c])
    c_bias = [local(bu_ref, bu), local(bv_ref, bv), local(pos_ref, posv)]
    c_k = local(kc_ref, kc)
    c_v = local(vc_ref, vc)
    c_wo = local(wout_ref, wo_land.at[c])
    c_up = local(wup_ref.at[:, lanes(fx, x)], wup.at[w])
    c_dn = local(wdn_ref, wdn.at[c])
    for cp in c_rel:
        cp.wait()
    tab = jnp.where(c == 0, relt[:, :ds], relt[:, ds:])
    hs = n_slots // 2
    rsend[...] = dot(tab, wrel[...], NT).reshape(2, hs, hw)
    for cp in c_small:
        cp.wait()
    gall[w, 0:1, :] = ga[...].reshape(1, ds)
    gall[w, 1:2, :] = gm[...].reshape(1, ds)

    pl.semaphore_wait(barrier, len(peers))

    hq = qr // 2

    def tok_unit(xx, yy, h):
        return xall.at[xx, rowsl(yy * qr + h * hq, hq)]

    def tok_x(xx, h):
        return tok_unit(xx, y, h)

    c_x.wait()
    x_start("tx", tok_x)
    send(wqkv_ref.at[:, :, 1 - c], wq_land.at[c], sib, "wqs")
    send(gall.at[w], gall.at[w], sib, ("g", 0))
    for i in range(1, nx):
        send(gall.at[w], gall.at[w], dev(xp(i), c, y), ("g", i))
    send(rsend.at[1 - c], rsib, sib, "r0")
    x_relay("tx", tok_x, "L")
    y_send("ty", tok_unit, "L", 0)
    x_relay("tx", tok_x, "R")
    y_send("ty", tok_unit, "R", 1)
    c_wq.wait()
    arrived(wq_land.at[1 - c], "wqs")
    for s in range(3):
        for j in range(nx):
            wpk[j, s * hd:(s + 1) * hd, :] = jnp.concatenate([wq_land[0, s, j], wq_land[1, s, j]], axis=1)

    def wq_unit(cc, xx):
        return wq.at[rowsl(cc * (3 * hd), 3 * hd), lanes(dx, xx)]

    for i, key in ((1, "L"), (nx - 1, "R"), (2, "O")):
        send(wpk.at[xp(i)], wq_unit(c, x), dev(xp(i), c, y), ("wx", key))
    wq[rowsl(c * (3 * hd), 3 * hd), lanes(dx, x)] = wpk[x]
    send(wpk.at[x], wq_unit(c, x), sib, ("ws", "S"))
    arrived(rsib, "r0")
    rland[x] = rsend[c] + rsib[...]
    for i, key in ((1, "L"), (nx - 1, "R"), (2, "O")):
        send(rland.at[x], rland.at[x], dev(xp(i), c, y), ("r1", key))
    for frm, h in (("L", 1), ("R", 0), ("O", 0), ("O", 1)):
        x_wait("tx", tok_x, frm, h)
        y_send("ty", tok_unit, frm, h)

    def up_send(p):
        r0, r1 = UP_PARTS[p], UP_PARTS[p + 1]
        for i, key in ((1, "L"), (nx - 1, "R"), (2, "O")):
            send(wup_ref.at[r0:r1, lanes(fx, xp(i))], wup.at[w, r0:r1], dev(xp(i), c, y), ("ux", p, key))

    def up_relay(p):
        r0, r1 = UP_PARTS[p], UP_PARTS[p + 1]
        for key in "LRO":
            blk = wup.at[2 * xof[key] + c, r0:r1]
            arrived(blk, ("ux", p, key))
            send(blk, blk, sib, ("us", p, key))

    up_send(0)
    send(wout_ref, wo_land.at[c], sib, "wo")
    send(wdn_ref, wdn.at[c], sib, "dn")
    send(wup_ref.at[:, lanes(fx, x)], wup.at[w], sib, "uown")
    for i in range(1, nx):
        blk = gall.at[2 * lax.rem(x + nx - i, nx) + c]
        arrived(blk, ("g", i))
        send(blk, blk, sib, ("gs", i))
    arrived(gall.at[2 * x + 1 - c], ("g", 0))
    for i in range(1, nx):
        arrived(gall.at[2 * lax.rem(x + nx - i, nx) + 1 - c], ("gs", i))
    gain[...] = jnp.concatenate([gall[j, 0:1, :] for j in range(2 * nx)], axis=1)
    def norm_block(px, yy):
        v = xall[xof[px], rowsl(yy * qr, qr), :].astype(F32)
        ms = jnp.mean(v * v, axis=-1, keepdims=True)
        nall[rowsl("ORLS".index(px) * rows + yy * qr, qr), :] = (v * lax.rsqrt(ms + NORM_EPS) * gain[...]).astype(BF16)

    def norm_own(r, carry):
        norm_block("S", r)
        return carry

    lax.fori_loop(0, ny, norm_own, 0)
    for px in "LRO":
        norm_block(px, y)
    for px, frm in (("L", "D"), ("R", "U"), ("L", "U"), ("R", "D"), ("O", "D"), ("O", "U")):
        y_relay("ty", tok_unit, px, frm)
    for px in "LRO":
        y_wait("ty", tok_unit, px, "D", 1)
        norm_block(px, yof["D"])
        y_wait("ty", tok_unit, px, "U", 0)
        norm_block(px, yof["U"])
    def qkv_part(key, p):
        k = lanes(dx, xof[key])
        return dot(wq[:, k], nall[2 * p * rows:2 * (p + 1) * rows, k], NT)

    def wq_relay(key):
        arrived(wq_unit(c, xof[key]), ("wx", key))
        send(wq_unit(c, xof[key]), wq_unit(c, xof[key]), sib, ("ws", key))

    wq_relay("L")
    wq_relay("R")
    wq_relay("O")
    for px in "LRO":
        y_wait("ty", tok_unit, px, "O", 0)
        y_wait("ty", tok_unit, px, "O", 1)
        norm_block(px, yof["O"])
    arrived(wq_unit(1 - c, x), ("ws", "S"))
    for p in range(2):
        qacc[p] = qkv_part("S", p)
    for key in "LR":
        arrived(wq_unit(1 - c, xof[key]), ("ws", key))
    for p in range(2):
        qacc[p] += qkv_part("L", p) + qkv_part("R", p)
    arrived(wq_unit(1 - c, xof["O"]), ("ws", "O"))
    for p, pair in enumerate((((2, "O"), (1, "L")), ((nx - 1, "R"), (0, "S")))):
        res = (qacc[p] + qkv_part("O", p)).astype(BF16).reshape(hx, 3, hd, 2 * rows)
        for k, (i, key) in enumerate(pair):
            if i:
                qst[i - 1] = res[:, :, :, k * rows:(k + 1) * rows]
                send(qst.at[i - 1, :, 0:2], qin.at[x, :, 0:2], dev(xp(i), c, y), ("q", key))
            else:
                qin[x] = res[:, :, :, k * rows:(k + 1) * rows]
    for i, key in ((2, "O"), (1, "L"), (nx - 1, "R")):
        send(qst.at[i - 1, :, 2], qin.at[x, :, 2], dev(xp(i), c, y), ("v", key))
    up_send(1)
    for key in "LRO":
        arrived(rland.at[xof[key]], ("r1", key))
    rel = rland[0]
    for j in range(1, nx):
        rel = rel + rland[j]
    rfull[c] = rel
    send(rfull.at[c], rfull.at[c], sib, "r2")
    up_relay(0)
    arrived(rfull.at[1 - c], "r2")
    rel = rfull[...].reshape(n_slots, hw).astype(BF16).astype(F32)
    rel = jnp.broadcast_to(rel[:, None, :], (n_slots, n_heads, hw)).reshape(n_slots * n_heads, hw)
    col = lax.broadcasted_iota(jnp.int32, rel.shape, 1)
    row_head = lax.rem(lax.broadcasted_iota(jnp.int32, rel.shape, 0), n_heads)
    keep = (col >= row_head * hd) & (col < row_head * hd + hd)
    rel_diag[...] = jnp.where(keep, rel, 0.0).astype(BF16)
    c_k.wait()
    for key in "LRO":
        arrived(qin.at[xof[key], :, 0:2], ("q", key))
    outs = []
    for j in range(nx):
        outs.append(local(qin.at[j, :, 1], kn_ref.at[j * hx:(j + 1) * hx]))
    for cp in c_bias:
        cp.wait()
    pos = posv[...]
    bu_t, bv_t = bu[...].T, bv[...].T
    scale = 1.0 / math.sqrt(hd)
    selfs, qvs = [], []
    for h in range(n_heads):
        q = qin[h // hx, h % hx, 0].astype(F32)
        qu = (q + bu_t[:, h:h + 1]).astype(BF16).astype(F32)
        qvs.append((q + bv_t[:, h:h + 1]).astype(BF16))
        selfs.append(jnp.sum(qu * qin[h // hx, h % hx, 1].astype(F32), axis=0, keepdims=True))
        for j in range(n_slots):
            s_ref[j, h:h + 1, :] = jnp.sum(kc[h, j].astype(F32) * qu, axis=0, keepdims=True)
    self_score = jnp.concatenate(selfs, axis=0)
    rel_all = dot(rel_diag[...], jnp.concatenate(qvs, axis=0), NN)
    rel_all = [rel_all[r * n_heads:(r + 1) * n_heads] for r in range(n_slots)][::-1]
    shift = n_slots - 1 - pos
    bit = 1
    while bit < n_slots:
        take = (shift // bit) % 2 == 1
        rel_all = [jnp.where(take, rel_all[j + bit], rel_all[j]) if j + bit < n_slots else rel_all[j] for j in range(n_slots)]
        bit *= 2
    sc = []
    for j in range(n_slots):
        content = jnp.where(pos == j, self_score, s_ref[j])
        sc.append(jnp.where(pos >= j, (content + rel_all[j]) * scale, -1e30))
    top = functools.reduce(jnp.maximum, sc)
    ex = [jnp.exp(v - top) for v in sc]
    tot = functools.reduce(jnp.add, ex)
    probs = [(v / tot).astype(BF16).astype(F32) for v in ex]
    self_prob = functools.reduce(jnp.add, [jnp.where(pos == j, probs[j], 0.0) for j in range(n_slots)])
    for j in range(n_slots):
        p_ref[j] = jnp.where(pos == j, 0.0, probs[j])
    p_ref[n_slots] = self_prob
    c_v.wait()
    for key in "LRO":
        arrived(qin.at[xof[key], :, 2], ("v", key))
    for j in range(nx):
        outs.append(local(qin.at[j, :, 2], vn_ref.at[j * hx:(j + 1) * hx]))
    for h in range(n_heads):
        acc = p_ref[n_slots, h:h + 1, :] * qin[h // hx, h % hx, 2].astype(F32)
        for j in range(n_slots):
            acc = acc + p_ref[j, h:h + 1, :] * vc[h, j].astype(F32)
        o_t[h * hd:(h + 1) * hd, :] = acc
    oall[x] = o_t[...].T.astype(BF16)
    half = rows // 2

    oq = rows // 4

    def o_unit(px, k0, n):
        return oall.at[xof[px], k0 * oq:(k0 + n) * oq]

    for k0, n, to, frm in ((0, 1, right, "L"), (2, 1, left, "R"), (1, 1, right, "L"), (3, 1, left, "R"), (2, 2, right, "L"), (0, 2, left, "R")):
        send(o_unit("S", k0, n), o_unit("S", k0, n), to, ("o", frm, k0))
    c_wo.wait()
    arrived(wo_land.at[1 - c], "wo")
    wo[...] = jnp.concatenate([wo_land[0], wo_land[1]], axis=1)

    def out_proj(px):
        g = xof[px]
        part = dot(oall[g], wo[...], NN).astype(BF16)
        st1[g] = part.reshape(ny, qr, dx)
        for i, key in ((2, "O"), (1, "D"), (ny - 1, "U")):
            send(st1.at[g, yp(i)], in1.at[y, g], dev(x, c, yp(i)), ("r1y", px, key))
        in1[y, g] = st1[g, y]

    out_proj("S")
    for frm, k, to in (("L", 0, right), ("R", 2, left), ("L", 1, right), ("R", 3, left)):
        arrived(o_unit(frm, k, 1), ("o", frm, k))
        send(o_unit(frm, k, 1), o_unit(frm, k, 1), to, ("o", "O", k))
    up_send(2)
    arrived(o_unit("L", 2, 2), ("o", "L", 2))
    out_proj("L")
    arrived(o_unit("R", 0, 2), ("o", "R", 0))
    out_proj("R")
    for k in range(4):
        arrived(o_unit("O", k, 1), ("o", "O", k))
    out_proj("O")
    up_relay(1)
    gain_m = jnp.concatenate([gall[2 * x, 1:2, :], gall[2 * x + 1, 1:2, :]], axis=1)
    for px in "SLRO":
        for key in "DUO":
            arrived(in1.at[yof[key], xof[px]], ("r1y", px, key))
    for g in range(nx):
        acc = in1[0, g].astype(F32)
        for k in range(1, ny):
            acc = acc + in1[k, g].astype(F32)
        acc = xall[g, rowsl(y * qr, qr), lanes(dx, x)].astype(F32) + acc
        for k in range(2):
            hbuf[k * half + g * hq:k * half + (g + 1) * hq, :] = acc[k * hq:(k + 1) * hq]
    h = hbuf[...]
    sq = jnp.sum(h * h, axis=1, keepdims=True)
    sq = jnp.broadcast_to(sq, (rows, rows)).T[:8]
    st_s[...] = sq
    st_r[x] = sq
    for i, key in ((2, "O"), (1, "L"), (nx - 1, "R")):
        send(st_s, st_r.at[x], dev(xp(i), c, y), ("st", key))
    up_send(3)
    for key in "LRO":
        arrived(st_r.at[xof[key]], ("st", key))
    tot = st_r[0]
    for j in range(1, nx):
        tot = tot + st_r[j]
    rstd = lax.rsqrt(tot * (1.0 / d_model) + NORM_EPS)
    rstd = jnp.broadcast_to(rstd[0:1], (rows, rows)).T[:, 0:1]
    mall[y, :, lanes(dx, x)] = (hbuf[...] * rstd * gain_m).astype(BF16)

    sub = half // 2

    def piece(h, k=None):
        return slice(h * half, (h + 1) * half) if k is None else slice(h * half + k * sub, h * half + (k + 1) * sub)

    def m_unit(px, py, h, k=None):
        return mall.at[yof[py], piece(h, k), lanes(dx, xof[px])]

    def z_unit(px, py, h, k=None):
        return zall.at[yof[py], piece(h, k), lanes(fx, xof[px])]

    def xs_send(name, unit, py, h):
        blk = unit("S", py, h)
        send(blk, blk, right, (name, py, h, "L"))
        send(blk, blk, left, (name, py, h, "R"))

    direct = set()

    def xs_direct(name, unit, py, h):
        direct.add((name, py, h))
        blk = unit("S", py, h)
        send(blk, blk, dev(xp(2), c, y), (name, py, h, "O"))
        xs_send(name, unit, py, h)

    def xs_near(name, unit, py, h):
        for frm in "LR":
            arrived(unit(frm, py, h), (name, py, h, frm))

    def xs_relay(name, unit, py, h):
        for frm, to, k in (("L", right, 0), ("R", left, 1)):
            arrived(unit(frm, py, h), (name, py, h, frm))
            blk = unit(frm, py, h, k)
            send(blk, blk, to, (name, py, h, "O", k))

    def xs_last(name, unit, py, h):
        if (name, py, h) in direct:
            arrived(unit("O", py, h), (name, py, h, "O"))
            return
        for k in range(2):
            arrived(unit("O", py, h, k), (name, py, h, "O", k))

    def ys_send(px, h):
        blk = m_unit(px, "S", h)
        send(blk, blk, above, ("my", px, h, "D"))
        send(blk, blk, below, ("my", px, h, "U"))

    def ys_relay(px, h):
        for frm, to, k in (("D", above, 0), ("U", below, 1)):
            arrived(m_unit(px, frm, h), ("my", px, h, frm))
            blk = m_unit(px, frm, h, k)
            send(blk, blk, to, ("my", px, h, "O", k))

    def ys_last(h):
        for px in "SLRO":
            for k in range(2):
                arrived(m_unit(px, "O", h, k), ("my", px, h, "O", k))

    def hidden(blocks, spread=xs_send):
        m = jnp.concatenate([mall[yof[py], piece(h), :] for py, h in blocks], axis=0)
        z = dot(m, wup[...].reshape(d_model, fx), NN)
        z = jax.nn.gelu(z, approximate=True).astype(BF16)
        for k, (py, h) in enumerate(blocks):
            zall[yof[py], piece(h), lanes(fx, x)] = z[k * half:(k + 1) * half]
            spread("z", z_unit, py, h)

    def down(blocks):
        for py, h in blocks:
            xs_last("z", z_unit, py, h)
        z = jnp.concatenate([zall[yof[py], piece(h), :] for py, h in blocks], axis=0)
        part = dot(z, wdn[...].reshape(dx, ff), NT).astype(BF16)
        for k, (py, h) in enumerate(blocks):
            blk = part[k * half:(k + 1) * half]
            if py == "S":
                in2[y, h] = blk
            else:
                j = "DUO".index(py)
                st2[j, h] = blk
                send(st2.at[j, h], in2.at[y, h], dev(x, c, yof[py]), ("r2y", {"D": "U", "U": "D", "O": "O"}[py], h))

    def y_unit(px, h):
        return yfull.at[h * hq:(h + 1) * hq, lanes(dx, xof[px])]

    def y_out(px, py, h):
        return y_ref.at[yof[py], h * hq:(h + 1) * hq, lanes(dx, xof[px])]

    def yy_send(px, h):
        for i, key in ((2, "O"), (1, "D"), (ny - 1, "U")):
            send(y_unit(px, h), y_out(px, "S", h), dev(x, c, yp(i)), ("yy", px, h, key))
        outs.append(local(y_unit(px, h), y_out(px, "S", h)))

    def finish(h):
        for key in "DUO":
            arrived(in2.at[yof[key], h], ("r2y", key, h))
        acc = in2[0, h].astype(F32)
        for k in range(1, ny):
            acc = acc + in2[k, h].astype(F32)
        yst[h] = (hbuf[piece(h), :] + acc).astype(BF16).reshape(nx, hq, dx)
        for i, key in ((2, "O"), (1, "L"), (nx - 1, "R")):
            send(yst.at[h, xp(i)], y_unit("S", h), dev(xp(i), c, y), ("yx", key, h))
        yfull[h * hq:(h + 1) * hq, lanes(dx, x)] = yst[h, x]
        yy_send("S", h)

    def y_forward(h):
        for px in "LRO":
            arrived(y_unit(px, h), ("yx", px, h))
            yy_send(px, h)

    xs_direct("mx", m_unit, "S", 0)
    ys_send("S", 0)
    xs_direct("mx", m_unit, "S", 1)
    ys_send("S", 1)
    up_relay(2)
    up_relay(3)
    xs_last("mx", m_unit, "S", 0)
    ys_send("O", 0)
    xs_near("mx", m_unit, "S", 0)
    ys_send("L", 0)
    ys_send("R", 0)
    c_up.wait()
    arrived(wup.at[2 * x + 1 - c], "uown")
    for p in range(4):
        for key in "LRO":
            arrived(wup.at[2 * xof[key] + 1 - c, UP_PARTS[p]:UP_PARTS[p + 1]], ("us", p, key))
    hidden([("S", 0)], xs_direct)
    xs_last("mx", m_unit, "S", 1)
    xs_near("mx", m_unit, "S", 1)
    hidden([("S", 1)], xs_direct)
    for px in "SOLR":
        ys_relay(px, 0)
    for px in "OLR":
        ys_send(px, 1)
    hidden([("D", 0), ("U", 0)])
    ys_last(0)
    hidden([("O", 0)])
    for px in "SLRO":
        ys_relay(px, 1)
    xs_relay("z", z_unit, "D", 0)
    xs_relay("z", z_unit, "U", 0)
    hidden([("D", 1), ("U", 1)])
    c_dn.wait()
    arrived(wdn.at[1 - c], "dn")
    xs_near("z", z_unit, "S", 0)
    xs_near("z", z_unit, "S", 1)
    down([("S", 0), ("S", 1)])
    xs_relay("z", z_unit, "O", 0)
    ys_last(1)
    hidden([("O", 1)])
    down([("D", 0), ("U", 0)])
    xs_relay("z", z_unit, "D", 1)
    xs_relay("z", z_unit, "U", 1)
    down([("O", 0)])
    xs_relay("z", z_unit, "O", 1)
    down([("D", 1), ("U", 1)])
    down([("O", 1)])
    finish(0)
    y_forward(0)
    finish(1)
    y_forward(1)
    for h in range(2):
        for px in "SLRO":
            for key in "DUO":
                arrived(y_out(px, key, h), ("yy", px, h, key))
    for cp in pending:
        cp.wait_send()
    for cp in outs:
        cp.wait()
    assert len(ids) <= N_REMOTE and n_local[0] <= N_LOCAL


def copy_kernel(*refs):
    n = (len(refs) - 1) // 3
    srcs, dsts, bufs, sems = refs[:n], refs[n:2 * n], refs[2 * n:3 * n], refs[3 * n]
    ins = [pltpu.make_async_copy(srcs[i], bufs[i], sems.at[i]) for i in range(n)]
    outs = [pltpu.make_async_copy(bufs[i], dsts[i], sems.at[n + i]) for i in range(n)]
    for cp in ins:
        cp.start()
    for i in range(n):
        ins[i].wait()
        outs[i].start()
    for cp in outs:
        cp.wait()


def copy_out(*arrays):
    n = len(arrays)
    any_spec = pl.BlockSpec(memory_space=pl.ANY)
    return pl.pallas_call(
        copy_kernel,
        out_shape=tuple(jax.ShapeDtypeStruct(a.shape, a.dtype) for a in arrays),
        in_specs=[any_spec] * n,
        out_specs=tuple([any_spec] * n),
        scratch_shapes=[pltpu.VMEM(a.shape, a.dtype) for a in arrays] + [pltpu.SemaphoreType.DMA((2 * n,))],
    )(*arrays)


def solution(mesh):
    nx, ny = mesh.shape["wg"] // 2, mesh.shape["tp"]
    tok_axes = ("dp", "wg")
    in_specs = (P(tok_axes, None), P("wg"), P("wg"), P("wg", None, "tp", None), P("wg", "tp", None), P("tp", None, "wg"), P("wg", "tp"), P("tp", "wg"), P("tp", None), P("tp", None), P(None, None), P(tok_axes, "tp", None, None), P(tok_axes, "tp", None, None), P(tok_axes))
    out_specs = (P(tok_axes, None), P(tok_axes, "tp", None), P(tok_axes, "tp", None))

    def device_step(tokens, gain_attn, gain_mlp, w_qkv, w_rel, w_out, w_up, w_down, bias_u, bias_v, rel_table, k_cache, v_cache, positions):
        rows, d_model = tokens.shape
        ds = gain_attn.shape[0]
        dx = 2 * ds
        _, n_heads, n_slots, hd = k_cache.shape
        hx = n_heads // nx
        hw = n_heads * hd
        ff = w_up.shape[1]
        fx = ff // nx
        qr = rows // ny
        any_spec = pl.BlockSpec(memory_space=pl.ANY)
        vm = pltpu.VMEM
        scratch = [
            vm((nx, rows, d_model), BF16),
            vm((nx * rows, d_model), BF16),
            vm((2, 3 * hx * hd, 2 * rows), F32),
            vm((ds,), F32),
            vm((ds,), F32),
            vm((n_slots, dx), BF16),
            vm((n_heads, hd), F32),
            vm((n_heads, hd), F32),
            vm((1, rows), jnp.int32),
            vm((2 * nx, 2, ds), F32),
            vm((1, d_model), F32),
            vm((2, 3, nx, hd, ds), BF16),
            vm((nx, 3 * hd, dx), BF16),
            vm((hx * 3 * hd, d_model), BF16),
            vm((nx - 1, hx, 3, hd, rows), BF16),
            vm((nx, hx, 3, hd, rows), BF16),
            vm((n_heads, n_slots, hd, rows), BF16),
            vm((n_heads, n_slots, hd, rows), BF16),
            vm((hw, ds), BF16),
            vm((2, n_slots // 2, hw), F32),
            vm((n_slots // 2, hw), F32),
            vm((nx, n_slots // 2, hw), F32),
            vm((2, n_slots // 2, hw), F32),
            vm((n_slots * n_heads, hw), BF16),
            vm((n_slots, n_heads, rows), F32),
            vm((n_slots + 1, n_heads, rows), F32),
            vm((hw, rows), F32),
            vm((nx, rows, hw), BF16),
            vm((2, hw, ds), BF16),
            vm((hw, dx), BF16),
            vm((nx, ny, qr, dx), BF16),
            vm((ny, nx, qr, dx), BF16),
            vm((rows, dx), F32),
            vm((8, rows), F32),
            vm((nx, 8, rows), F32),
            vm((ny, rows, d_model), BF16),
            vm((2 * nx, ds, fx), BF16),
            vm((ny, rows, ff), BF16),
            vm((2, ds, ff), BF16),
            vm((ny - 1, 2, rows // 2, dx), BF16),
            vm((ny, 2, rows // 2, dx), BF16),
            vm((2, nx, qr // 2, dx), BF16),
            vm((qr, d_model), BF16),
            pltpu.SemaphoreType.DMA((N_REMOTE,)),
            pltpu.SemaphoreType.DMA((N_REMOTE,)),
            pltpu.SemaphoreType.DMA((N_LOCAL,)),
        ]
        y, kn, vn = pl.pallas_call(
            functools.partial(layer_kernel, nx, ny),
            out_shape=(
                jax.ShapeDtypeStruct((ny, qr, d_model), BF16),
                jax.ShapeDtypeStruct((n_heads, hd, rows), BF16),
                jax.ShapeDtypeStruct((n_heads, hd, rows), BF16),
            ),
            in_specs=[any_spec] * 14,
            out_specs=(any_spec, any_spec, any_spec),
            scratch_shapes=scratch,
            compiler_params=pltpu.CompilerParams(collective_id=0, has_side_effects=True, vmem_limit_bytes=60 * 2**20),
        )(
            tokens, gain_attn, gain_mlp, w_qkv.transpose(1, 2, 3, 0).reshape(3, nx, hx, hd, ds), w_rel.transpose(1, 2, 0).reshape(hw, ds), w_out.reshape(hw, ds),
            w_up, w_down.T, bias_u, bias_v, rel_table, k_cache.transpose(1, 2, 3, 0), v_cache.transpose(1, 2, 3, 0), positions[None, :],
        )
        y, kn, vn = copy_out(y.reshape(rows, d_model), kn, vn)
        return y, kn.transpose(2, 0, 1), vn.transpose(2, 0, 1)

    return jax.shard_map(device_step, mesh=mesh, in_specs=in_specs, out_specs=out_specs, check_vma=False)
```
